32 devices in a mesh: ep: 32 (over z, y, x, core).
Axes of the slice: x: 2, y: 2, z: 4, core: 2. Of those that a mesh axis runs over, the one named last changes fastest.
Arguments:
- tokens: bfloat16 [128, 64, 768], P('ep')
- loss_weight: bfloat16 [128, 64, 768], P('ep')
- w_gate: bfloat16 [768, 32], replicated
- w_in: bfloat16 [32, 768, 3072], P('ep')
- w_out: bfloat16 [32, 3072, 768], P('ep')
- first_expert: int32 [128, 64], P('ep')
- second_expert: int32 [128, 64], P('ep')
- keep_second: int32 [128, 64], P('ep')
Outputs:
- output 1: float32 [], replicated
- output 2: bfloat16 [128, 64, 768], P('ep')
- output 3: bfloat16 [32, 768, 3072], P('ep')
- output 4: bfloat16 [32, 3072, 768], P('ep')
- output 5: float32 [768, 32], replicated
All inputs are finite; a program needn't handle non-finite values.
Results may differ from the reference program's by a relative error of at most 0.00948372.
Values are sent between devices in bfloat16 or wider.
A program may use at most 1 GiB of HBM per device.

```python
import jax
import jax.numpy as jnp
from jax import lax

EXPERTS = 32
HIDDEN = 768
FF_DIM = 3072
SEQ_LEN = 64
GROUPS = 128
CAPACITY = 2 * SEQ_LEN // EXPERTS
TOKENS = GROUPS * SEQ_LEN
NUMEL = TOKENS * HIDDEN
ALPHA = 0.01


def draw_routes(route_key):
    sub_keys = jax.random.split(route_key, 6)
    skew_level = jax.random.randint(sub_keys[0], (GROUPS, 1), 0, 4)
    hot_expert = jax.random.randint(sub_keys[1], (GROUPS, 1), 0, EXPERTS)
    hot_pick = jax.random.randint(sub_keys[2], (GROUPS, SEQ_LEN), 0, 8)
    spread = jax.random.randint(sub_keys[3], (GROUPS, SEQ_LEN), 0, EXPERTS)
    first_expert = jnp.where(hot_pick < skew_level, hot_expert, spread).astype(jnp.int32)
    offset = jax.random.randint(sub_keys[4], (GROUPS, SEQ_LEN), 1, EXPERTS)
    second_expert = ((first_expert + offset) % EXPERTS).astype(jnp.int32)
    keep_second = (jax.random.randint(sub_keys[5], (GROUPS, SEQ_LEN), 0, 3) > 0).astype(jnp.int32)
    return first_expert, second_expert, keep_second


def setup_inputs(seed: int = 0) -> dict:
    sub_keys = jax.random.split(jax.random.key(seed), 6)
    tokens = jax.random.normal(sub_keys[0], (GROUPS, SEQ_LEN, HIDDEN), jnp.float32).astype(jnp.bfloat16)
    loss_weight = jax.random.normal(sub_keys[1], (GROUPS, SEQ_LEN, HIDDEN), jnp.float32).astype(jnp.bfloat16)
    w_gate = (jax.random.normal(sub_keys[2], (HIDDEN, EXPERTS), jnp.float32) * HIDDEN ** -0.5).astype(jnp.bfloat16)
    w_in = (jax.random.normal(sub_keys[3], (EXPERTS, HIDDEN, FF_DIM), jnp.float32) * HIDDEN ** -0.5).astype(jnp.bfloat16)
    w_out = (jax.random.normal(sub_keys[4], (EXPERTS, FF_DIM, HIDDEN), jnp.float32) * FF_DIM ** -0.5).astype(jnp.bfloat16)
    first_expert, second_expert, keep_second = draw_routes(sub_keys[5])
    return {'tokens': tokens, 'loss_weight': loss_weight, 'w_gate': w_gate, 'w_in': w_in, 'w_out': w_out, 'first_expert': first_expert, 'second_expert': second_expert, 'keep_second': keep_second}


def table_for(hot_rows, pos_rows, kept_rows):
    slot_ids = jnp.arange(CAPACITY, dtype=jnp.int32)
    slot_hit = ((pos_rows[:, None, None] == slot_ids) & (kept_rows[:, None, None] > 0)).astype(jnp.float32)
    return hot_rows[:, :, None] * slot_hit


def expert_apply(packed):
    x_slots, w_first, w_second = packed
    pre_act = jnp.einsum('gch,hf->gcf', x_slots.astype(jnp.float32), w_first.astype(jnp.float32))
    act_bf = jax.nn.gelu(pre_act, approximate=True).astype(jnp.bfloat16)
    return jnp.einsum('gcf,fh->gch', act_bf.astype(jnp.float32), w_second.astype(jnp.float32)).astype(jnp.bfloat16)


def reference(tokens, loss_weight, w_gate, w_in, w_out, first_expert, second_expert, keep_second):
    expert_ids = jnp.arange(EXPERTS, dtype=jnp.int32)
    first_int = (first_expert[..., None] == expert_ids).astype(jnp.int32)
    second_int = (second_expert[..., None] == expert_ids).astype(jnp.int32)
    second_keep = second_int * keep_second[..., None]
    first_count = jnp.sum(first_int, axis=1)
    pos_first = jnp.sum((jnp.cumsum(first_int, axis=1) - first_int) * first_int, axis=-1)
    pos_second = jnp.sum((jnp.cumsum(second_keep, axis=1) - second_keep + first_count[:, None, :]) * second_int, axis=-1)
    kept_first = (pos_first < CAPACITY).astype(jnp.int32)
    kept_second = keep_second * (pos_second < CAPACITY).astype(jnp.int32)
    first_hot = first_int.astype(jnp.float32)
    second_hot = second_int.astype(jnp.float32)
    frac_first = jnp.sum(first_hot, axis=(0, 1)) / TOKENS

    def dispatch_group(packed):
        x_group, pos_one, kept_one, hot_one, pos_two, kept_two, hot_two = packed
        table = table_for(hot_one, pos_one, kept_one) + table_for(hot_two, pos_two, kept_two)
        return jnp.einsum('sec,sh->ech', table, x_group).astype(jnp.bfloat16)

    def combine_group(packed):
        y_group, pos_one, kept_one, hot_one, pos_two, kept_two, hot_two, norm_one, norm_two = packed
        combine = (table_for(hot_one, pos_one, kept_one) * norm_one[:, None, None] + table_for(hot_two, pos_two, kept_two) * norm_two[:, None, None]).astype(jnp.bfloat16)
        return jnp.einsum('sec,ech->sh', combine.astype(jnp.float32), y_group.astype(jnp.float32))

    def objective(x_in, gate_w, w_first, w_second):
        x_f32 = x_in.astype(jnp.float32)
        logits = jnp.einsum('gsh,he->gse', x_f32, gate_w)
        router_prob = jax.nn.softmax(logits, axis=-1)
        gate_first = jnp.sum(router_prob * first_hot, axis=-1)
        gate_second = jnp.sum(router_prob * second_hot, axis=-1)
        norm_first = gate_first / (gate_first + gate_second)
        norm_second = gate_second / (gate_first + gate_second)
        slots_in = lax.map(jax.checkpoint(dispatch_group), (x_f32, pos_first, kept_first, first_hot, pos_second, kept_second, second_hot))
        slots_out = lax.map(jax.checkpoint(expert_apply), (jnp.moveaxis(slots_in, 0, 1), w_first, w_second))
        moe_out = lax.map(jax.checkpoint(combine_group), (jnp.moveaxis(slots_out, 0, 1), pos_first, kept_first, first_hot, pos_second, kept_second, second_hot, norm_first, norm_second))
        dot_sum = jnp.sum((x_f32 + moe_out) * loss_weight.astype(jnp.float32))
        mean_prob = jnp.sum(router_prob, axis=(0, 1)) / TOKENS
        loss_value = dot_sum / NUMEL + ALPHA * EXPERTS * jnp.sum(frac_first * mean_prob)
        return loss_value * NUMEL, loss_value

    _, pull_back, loss_value = jax.vjp(objective, tokens, w_gate.astype(jnp.float32), w_in, w_out, has_aux=True)
    grad_x, grad_gate, grad_w_in, grad_w_out = pull_back(jnp.ones((), jnp.float32))
    return loss_value, grad_x, grad_w_in, grad_w_out, grad_gate
```

```python
import jax
import jax.numpy as jnp
from jax import lax
from jax.sharding import PartitionSpec as P

ALPHA = 0.01


def gelu_bf16(pre_act):
    return jax.nn.gelu(pre_act, approximate=True).astype(jnp.bfloat16)


def route_masks(first_ids, second_ids, keep_ids, experts, cap_rows):
    seq_len = first_ids.shape[1]
    expert_ids = jnp.arange(experts, dtype=jnp.int32)
    first_hot = (first_ids[..., None] == expert_ids).astype(jnp.bfloat16)
    second_hot = (second_ids[..., None] == expert_ids).astype(jnp.bfloat16)
    second_kept = second_hot * keep_ids.astype(jnp.bfloat16)[..., None]
    seq_ids = jnp.arange(seq_len, dtype=jnp.int32)
    earlier = (seq_ids[:, None] > seq_ids[None, :]).astype(jnp.bfloat16)
    before_first = jnp.einsum('st,gte->gse', earlier, first_hot, preferred_element_type=jnp.float32)
    before_second = jnp.einsum('st,gte->gse', earlier, second_kept, preferred_element_type=jnp.float32)
    first_count = jnp.sum(first_hot, axis=1, dtype=jnp.float32)
    pos_first = jnp.sum(before_first * first_hot, axis=-1)
    pos_second = jnp.sum((before_second + first_count[:, None, :]) * second_hot, axis=-1)
    slot_ids = jnp.arange(cap_rows, dtype=jnp.float32)
    disp_first = first_hot[..., None] * (pos_first[..., None, None] == slot_ids).astype(jnp.bfloat16)
    disp_second = second_kept[..., None] * (pos_second[..., None, None] == slot_ids).astype(jnp.bfloat16)
    return first_hot, second_hot, first_count, disp_first, disp_second


def solution(mesh):
    ep_size = mesh.shape['ep']

    def layer_body(x_loc, r_loc, w_gate, w_in_loc, w_out_loc, first_ids, second_ids, keep_ids):
        local_groups, seq_len, hidden = x_loc.shape
        experts = w_gate.shape[1]
        cap_rows = 2 * seq_len // experts
        tokens_all = local_groups * ep_size * seq_len
        numel = tokens_all * hidden
        first_hot, second_hot, first_count, disp_first, disp_second = route_masks(first_ids, second_ids, keep_ids, experts, cap_rows)
        logits = jnp.einsum('gsh,he->gse', x_loc, w_gate, preferred_element_type=jnp.float32)
        router_prob = jax.nn.softmax(logits, axis=-1)
        gate_first = jnp.sum(router_prob * first_hot, axis=-1)
        gate_second = jnp.sum(router_prob * second_hot, axis=-1)
        gate_sum = gate_first + gate_second
        norm_first = (gate_first / gate_sum).astype(jnp.bfloat16)
        norm_second = (gate_second / gate_sum).astype(jnp.bfloat16)
        dispatch = disp_first + disp_second
        combine = disp_first * norm_first[..., None, None] + disp_second * norm_second[..., None, None]
        send_x = jnp.einsum('gsec,gsh->egch', dispatch, x_loc, preferred_element_type=jnp.float32).astype(jnp.bfloat16)
        send_r = jnp.einsum('gsec,gsh->egch', dispatch, r_loc, preferred_element_type=jnp.float32).astype(jnp.bfloat16)
        send_n = jnp.einsum('gsec->egc', combine).astype(jnp.bfloat16)
        send_n = jnp.broadcast_to(send_n[..., None], send_n.shape + (128,))
        recv = lax.all_to_all(jnp.concatenate([send_x, send_r, send_n], axis=-1), 'ep', 0, 1, tiled=True)
        expert_x, expert_r, expert_n = recv[..., :hidden], recv[..., hidden:2 * hidden], recv[..., 2 * hidden:2 * hidden + 1]
        pre_act = jnp.einsum('egch,ehf->egcf', expert_x, w_in_loc, preferred_element_type=jnp.float32)
        act_bf, act_pull = jax.vjp(gelu_bf16, pre_act)
        expert_y = jnp.einsum('egcf,efh->egch', act_bf, w_out_loc, preferred_element_type=jnp.float32).astype(jnp.bfloat16)
        dots = jnp.sum(expert_y.astype(jnp.float32) * expert_r.astype(jnp.float32), axis=-1)
        dot_sum = jnp.einsum('gsh,gsh->', x_loc, r_loc, preferred_element_type=jnp.float32) + jnp.sum(dots * expert_n[..., 0].astype(jnp.float32))
        local_stats = jnp.concatenate([jnp.sum(first_count, axis=0), jnp.sum(router_prob, axis=(0, 1)), dot_sum[None]])
        global_stats = jnp.sum(lax.optimization_barrier(lax.all_gather(local_stats, 'ep')), axis=0)
        frac_first = global_stats[:experts] / tokens_all
        mean_prob = global_stats[experts:2 * experts] / tokens_all
        loss_value = global_stats[2 * experts] / numel + ALPHA * experts * jnp.sum(frac_first * mean_prob)

        grad_y = (expert_n.astype(jnp.float32) * expert_r.astype(jnp.float32)).astype(jnp.bfloat16)
        grad_act = jnp.einsum('egch,efh->egcf', grad_y, w_out_loc, preferred_element_type=jnp.float32).astype(jnp.bfloat16)
        grad_pre = act_pull(grad_act)[0].astype(jnp.bfloat16)
        grad_slots = jnp.einsum('egcf,ehf->egch', grad_pre, w_in_loc, preferred_element_type=jnp.float32).astype(jnp.bfloat16)
        grad_back = lax.all_to_all(grad_slots, 'ep', 1, 0, tiled=True)
        dots_back = lax.all_to_all(dots, 'ep', 1, 0, tiled=True)
        grad_w_out = jnp.einsum('egcf,egch->efh', act_bf, grad_y, preferred_element_type=jnp.float32).astype(jnp.bfloat16)
        grad_w_in = jnp.einsum('egch,egcf->ehf', expert_x, grad_pre, preferred_element_type=jnp.float32).astype(jnp.bfloat16)
        grad_x_moe = jnp.einsum('gsec,egch->gsh', dispatch, grad_back, preferred_element_type=jnp.float32)
        dots_slot = jnp.moveaxis(dots_back, 0, 1)[:, None]
        grad_norm_first = jnp.sum(disp_first * dots_slot, axis=(2, 3)).astype(jnp.bfloat16).astype(jnp.float32)
        grad_norm_second = jnp.sum(disp_second * dots_slot, axis=(2, 3)).astype(jnp.bfloat16).astype(jnp.float32)
        gate_sq = gate_sum * gate_sum
        grad_gate_first = (grad_norm_first - grad_norm_second) * gate_second / gate_sq
        grad_gate_second = (grad_norm_second - grad_norm_first) * gate_first / gate_sq
        grad_prob = grad_gate_first[..., None] * first_hot + grad_gate_second[..., None] * second_hot + (ALPHA * hidden * experts) * frac_first
        grad_logits = router_prob * (grad_prob - jnp.sum(router_prob * grad_prob, axis=-1, keepdims=True))
        grad_logits_bf = grad_logits.astype(jnp.bfloat16)
        grad_x_router = jnp.einsum('gse,he->gsh', grad_logits_bf, w_gate, preferred_element_type=jnp.float32)
        grad_x = (r_loc.astype(jnp.float32) + grad_x_moe + grad_x_router).astype(jnp.bfloat16)
        gate_part = jnp.einsum('gsh,gse->he', x_loc, grad_logits_bf, preferred_element_type=jnp.float32)
        gate_rows = jnp.sum(lax.all_to_all(gate_part.reshape(ep_size, -1, 128), 'ep', 0, 0), axis=0)
        grad_gate_w = lax.all_gather(gate_rows, 'ep').reshape(hidden, experts)
        return loss_value, grad_x, grad_w_in, grad_w_out, grad_gate_w

    row_spec = P('ep', None, None)
    id_spec = P('ep', None)
    return jax.shard_map(layer_body, mesh=mesh, in_specs=(row_spec, row_spec, P(None, None), row_spec, row_spec, id_spec, id_spec, id_spec), out_specs=(P(), row_spec, row_spec, row_spec, P(None, None)), check_vma=False)
```

```python
import functools

import jax
import jax.numpy as jnp
from jax import lax
from jax.experimental import pallas as pl
from jax.experimental.pallas import tpu as pltpu
from jax.sharding import PartitionSpec as P

ALPHA = 0.01
MESH = pl.DeviceIdType.MESH
F32 = jnp.float32
BF16 = jnp.bfloat16
NN = (((1,), (0,)), ((), ()))
NT = (((1,), (1,)), ((), ()))
TN = (((0,), (0,)), ((), ()))
GELU_C = 0.7978845608028654
GELU_K = 0.044715


def dot(a, b, dims=NN, **kw):
    return lax.dot_general(a, b, dims, preferred_element_type=F32, **kw)


def iota(shape, dim):
    return lax.broadcasted_iota(jnp.int32, shape, dim)


def flip_bits(a, b):
    return a + b - 2 * a * b


def layer_kernel(n, cap, seq, ids_ref, x_ref, r_ref, wg_ref, w1_hbm, w2_hbm,
                 loss_ref, gx_ref, gg_ref, gw1_hbm, gw2_hbm,
                 w1, w2, sx, sr, xe, re, gy, act, gpre, gs, gback, rows_s, rows_r, dots_s, dots_r,
                 part_s, part_r, sum_s, hacc, gacc, xet, stage1, stage2,
                 w_sem, out_sem, s_x, s_r, s_g, s_row, s_dot, s_part, s_sum,
                 v_x, v_r, v_g, v_row, v_dot, v_part, v_sum):
    me = lax.axis_index('ep')
    tokens, hidden = x_ref.shape
    ff = w1.shape[1]
    groups = tokens // seq
    rows = groups * cap
    slots = n * rows
    half = slots // 2
    plane = n // 4
    tokens_all = tokens * n
    numel = tokens_all * hidden
    tile = 512
    tiles = ff // tile

    low, high = lax.rem(me, plane), lax.div(me, plane)
    low_bits = [lax.rem(low, 2), lax.rem(lax.div(low, 2), 2), lax.div(low, 4)]
    high_bits = [lax.rem(high, 2), lax.div(high, 2)]
    order = (0, 2, 1, 3)

    def partner(quarter, step):
        far = order[quarter]
        top = [bit if not (far >> i) & 1 else 1 - bit for i, bit in enumerate(high_bits)]
        step_bits = [lax.rem(step, 2), lax.rem(lax.div(step, 2), 2), lax.div(step, 4)]
        bits = [flip_bits(a, b) for a, b in zip(low_bits, step_bits)]
        return (top[0] + 2 * top[1]) * plane + bits[0] + 2 * bits[1] + 4 * bits[2]

    def each_partner(quarters, body):
        for quarter in quarters:
            first = 1 if quarter == 0 else 0

            @pl.loop(first, plane)
            def _(step):
                body(quarter * plane + step, partner(quarter, step))

    everyone = (0, 1, 2, 3)
    quarters_of = ((0, 1), (2, 3))

    barrier = pltpu.get_barrier_semaphore()
    each_partner(everyone, lambda q, d: pl.semaphore_signal(barrier, inc=1, device_id=(d,), device_id_type=MESH))
    w1_copy = pltpu.make_async_copy(w1_hbm, w1, w_sem.at[0])
    w2_copy = pltpu.make_async_copy(w2_hbm, w2, w_sem.at[1])
    w1_copy.start()
    w2_copy.start()

    e1, e2, k2 = ids_ref[0:1, :], ids_ref[1:2, :], ids_ref[2:3, :]
    row_i, col_i = iota((tokens, tokens), 0), iota((tokens, tokens), 1)
    eye = row_i == col_i

    def column(row):
        return jnp.sum(jnp.where(eye, row, 0), axis=1, keepdims=True)

    e1c, e2c, k2c = column(e1), column(e2), column(k2)
    same_group = (row_i // seq) == (col_i // seq)
    earlier = same_group & (row_i < col_i)
    one = jnp.int32(1)
    pos1 = jnp.sum(jnp.where(earlier & (e1c == e1), one, 0), axis=0, keepdims=True)
    count1 = jnp.sum(jnp.where(same_group & (e1c == e2), one, 0), axis=0, keepdims=True)
    before2 = jnp.sum(jnp.where(earlier & (e2c == e2) & (k2c > 0), one, 0), axis=0, keepdims=True)
    pos2 = count1 + before2
    lane = iota((1, tokens), 1)
    group_base = (lane // seq) * cap
    kept1 = pos1 < cap
    kept2 = (pos2 < cap) & (k2 > 0)
    place1 = jnp.where(kept1, group_base + pos1, -1)
    place2 = jnp.where(kept2, group_base + pos2, -1)

    def slot_of(expert):
        apart = expert ^ me
        top = apart // plane
        swapped = (top // 2) + 2 * (top % 2)
        return swapped * plane + apart % plane

    key1 = jnp.where(kept1, slot_of(e1) * rows + place1, -1)
    key2 = jnp.where(kept2, slot_of(e2) * rows + place2, -1)
    slot_i = iota((slots, tokens), 0)
    disp = ((slot_i == key1) | (slot_i == key2)).astype(F32).astype(BF16)

    expert_i = iota((n, tokens), 0)
    hot1 = (expert_i == e1).astype(F32)
    hot2 = (expert_i == e2).astype(F32)
    place_i = iota((128, tokens), 0)
    at1 = (place_i == place1).astype(F32)
    at2 = (place_i == place2).astype(F32)

    x = x_ref[...]
    r = r_ref[...]
    wgt = wg_ref[...]
    logits = dot(wgt, x, NT)
    top_logit = jnp.max(logits, axis=0, keepdims=True)
    expd = jnp.exp(logits - top_logit)
    prob = expd / jnp.sum(expd, axis=0, keepdims=True)
    g1 = jnp.sum(prob * hot1, axis=0, keepdims=True)
    g2 = jnp.sum(prob * hot2, axis=0, keepdims=True)
    gsum = g1 + g2
    n1 = (g1 / gsum).astype(BF16).astype(F32)
    n2 = (g2 / gsum).astype(BF16).astype(F32)
    norm_rows = dot((hot1 * n1).astype(BF16), at1.astype(BF16), NT) + dot((hot2 * n2).astype(BF16), at2.astype(BF16), NT)
    sub_n, lane_n = iota((n, 128), 0), iota((n, 128), 1)

    def as_lanes(col, base):
        return jnp.sum(jnp.where(lane_n == sub_n + base, col, 0.0), axis=0, keepdims=True)

    def as_column(row, base):
        return jnp.sum(jnp.where(lane_n == sub_n + base, row, 0.0), axis=1, keepdims=True)

    xr = jnp.sum(jnp.sum(x.astype(F32) * r.astype(F32), axis=0, keepdims=True), axis=1, keepdims=True)
    lane_1 = iota((1, 128), 1)
    stats = as_lanes(jnp.sum(hot1, axis=1, keepdims=True), 32) + as_lanes(jnp.sum(prob, axis=1, keepdims=True), 64) + jnp.where(lane_1 == 96, xr, 0.0)
    rows_s[...] = norm_rows + stats

    sx[...] = dot(disp, x).astype(BF16)
    sr[...] = dot(disp, r).astype(BF16)

    pl.semaphore_wait(barrier, n - 1)

    def one_row(src, dst, src_row, send, recv, q, d):
        return pltpu.make_async_remote_copy(src.at[pl.ds(src_row, 1)], dst.at[pl.ds(me, 1)], send.at[q], recv.at[0], device_id=(d,), device_id_type=MESH)

    def block(src, dst, send, recv, half_i, q, d):
        at = pl.ds(q * rows, rows)
        return pltpu.make_async_remote_copy(src.at[at], dst.at[at], send.at[half_i], recv.at[half_i], device_id=(d,), device_id_type=MESH)

    def own_row(src, dst, src_row, recv):
        pltpu.make_async_copy(src.at[pl.ds(src_row, 1)], dst.at[pl.ds(me, 1)], recv.at[0]).start()

    def own_block(src, dst, recv):
        pltpu.make_async_copy(src.at[pl.ds(0, rows)], dst.at[pl.ds(0, rows)], recv.at[0]).start()

    def settle(ref, sem, rows_at):
        pltpu.make_async_copy(ref.at[rows_at], ref.at[rows_at], sem).wait()

    def half_at(c):
        return pl.ds(c * half, half)

    each_partner(everyone, lambda q, d: one_row(rows_s, rows_r, d, s_row, v_row, q, d).start())
    own_row(rows_s, rows_r, me, v_row)
    own_block(sx, xe, v_x)
    own_block(sr, re, v_r)
    for c in range(2):
        each_partner(quarters_of[c], lambda q, d: block(sx, xe, s_x, v_x, c, q, d).start())
        each_partner(quarters_of[c], lambda q, d: block(sr, re, s_r, v_r, c, q, d).start())

    settle(rows_r, v_row.at[0], pl.ds(0, n))
    all_rows = rows_r[...]
    total = jnp.sum(all_rows, axis=0, keepdims=True)
    frac = as_column(total, 32) / tokens_all
    mean_prob = as_column(total, 64) / tokens_all
    w1_copy.wait()
    w2_copy.wait()

    loss_part = jnp.zeros((1, 1), F32)
    for c in range(2):
        at = half_at(c)
        settle(xe, v_x.at[c], at)
        settle(re, v_r.at[c], at)
        slot_row = iota((half, n), 0) + c * half
        apart = slot_row // rows
        top = apart // plane
        source = (((top // 2) + 2 * (top % 2)) * plane + apart % plane) ^ me
        pick = (source == iota((half, n), 1)).astype(F32).astype(BF16)
        wide = dot(pick, all_rows.astype(BF16))
        mine = iota((half, 128), 1) == iota((half, 128), 0) % rows
        norm = jnp.sum(jnp.where(mine, wide, 0.0), axis=1, keepdims=True)
        xc = xe[at, :]
        rc = re[at, :].astype(F32)
        gy[at, :] = (norm * rc).astype(BF16)
        hacc[...] = jnp.zeros_like(hacc)
        gacc[...] = jnp.zeros_like(gacc)

        @pl.loop(0, tiles)
        def _(f):
            cols = pl.ds(pl.multiple_of(f * tile, tile), tile)
            w1t = w1[:, cols]
            w2t = w2[cols, :]
            pre = dot(xe[at, :], w1t)
            sq = pre * pre
            th = jnp.tanh(GELU_C * (pre + GELU_K * (sq * pre)))
            cdf = 0.5 * (1.0 + th)
            a = (pre * cdf).astype(BF16)
            slope = cdf + (0.5 * GELU_C) * pre * (1.0 - th * th) * (1.0 + 3 * GELU_K * sq)
            act[at, cols] = a
            hacc[...] += dot(a, w2t)
            ga = dot(gy[at, :], w2t, NT).astype(BF16)
            gp = (ga.astype(F32) * slope).astype(BF16)
            gpre[at, cols] = gp
            gacc[...] += dot(gp, w1t, NT)

        h = hacc[...].astype(BF16).astype(F32)
        d = jnp.sum(h * rc, axis=1, keepdims=True)
        loss_part = loss_part + jnp.sum(norm * d, axis=0, keepdims=True)
        spread = jnp.where(mine, d, 0.0)
        dots_s[pl.ds(c * (n // 2), n // 2), :] = jnp.sum(spread.reshape(n // 2, rows, 128), axis=1)
        gs[at, :] = gacc[...].astype(BF16)
        if c == 1:
            dots_s[...] = dots_s[...] + jnp.where(lane_1 == 16, loss_part, 0.0)
            each_partner(everyone, lambda q, d: one_row(dots_s, dots_r, q, s_dot, v_dot, q, d).start())
            own_row(dots_s, dots_r, 0, v_dot)
        else:
            own_block(gs, gback, v_g)
        each_partner(quarters_of[c], lambda q, d: block(gs, gback, s_g, v_g, c, q, d).start())

    def put1(f, slot):
        cols = pl.ds(pl.multiple_of(f * tile, tile), tile)
        return pltpu.make_async_copy(stage1.at[slot], gw1_hbm.at[:, cols], out_sem.at[slot])

    def put2(f, slot):
        cols = pl.ds(pl.multiple_of(f * tile, tile), tile)
        return pltpu.make_async_copy(stage2.at[slot], gw2_hbm.at[cols, :], out_sem.at[2 + slot])

    xet[...] = jnp.transpose(xe[...])

    @pl.loop(0, tiles)
    def _(f):
        slot = lax.rem(f, 2)

        @pl.when(f >= 2)
        def _():
            put1(f - 2, slot).wait()

        cols = pl.ds(pl.multiple_of(f * tile, tile), tile)
        stage1[slot] = dot(xet[...], gpre[:, cols]).astype(BF16)
        put1(f, slot).start()

    settle(dots_r, v_dot.at[0], pl.ds(0, n))
    all_dots = dots_r[...]
    exact = lax.Precision.HIGHEST
    d1 = jnp.sum(dot(all_dots, hot1, TN, precision=exact) * at1, axis=0, keepdims=True)
    d2 = jnp.sum(dot(all_dots, hot2, TN, precision=exact) * at2, axis=0, keepdims=True)
    d1 = d1.astype(BF16).astype(F32)
    d2 = d2.astype(BF16).astype(F32)
    gate_sq = gsum * gsum
    up1 = (d1 - d2) * g2 / gate_sq
    up2 = (d2 - d1) * g1 / gate_sq
    gprob = up1 * hot1 + up2 * hot2 + (ALPHA * hidden * n) * frac
    glog = (prob * (gprob - jnp.sum(prob * gprob, axis=0, keepdims=True))).astype(BF16)
    part_s[...] = dot(glog, x)
    each_partner(everyone, lambda q, d: one_row(part_s, part_r, d, s_part, v_part, q, d).start())
    own_row(part_s, part_r, me, v_part)

    both = jnp.sum(jnp.where(lane_1 == 96, total, 0.0), axis=1, keepdims=True)
    both = both + jnp.sum(jnp.where(lane_1 == 16, jnp.sum(all_dots, axis=0, keepdims=True), 0.0), axis=1, keepdims=True)
    aux = jnp.sum(frac * mean_prob, axis=0, keepdims=True) * n
    loss_ref[...] = jnp.broadcast_to(both / numel + ALPHA * aux, loss_ref.shape)

    @pl.loop(0, tiles)
    def _(f):
        slot = lax.rem(f, 2)

        @pl.when(f >= 2)
        def _():
            put2(f - 2, slot).wait()

        cols = pl.ds(pl.multiple_of(f * tile, tile), tile)
        stage2[slot] = dot(act[:, cols], gy[...], TN).astype(BF16)
        put2(f, slot).start()

    settle(part_r, v_part.at[0], pl.ds(0, n))
    sum_s[0:1, :] = jnp.sum(part_r[...], axis=0, keepdims=True)
    each_partner(everyone, lambda q, d: one_row(sum_s, gg_ref, 0, s_sum, v_sum, q, d).start())
    own_row(sum_s, gg_ref, 0, v_sum)

    key1c, key2c = column(key1), column(key2)
    slot_l = iota((tokens, slots), 1)
    comb = ((slot_l == key1c) | (slot_l == key2c)).astype(F32).astype(BF16)
    near = r.astype(F32) + dot(glog, wgt, TN)
    for c in range(2):
        settle(gback, v_g.at[c], half_at(c))
    gx_ref[...] = (near + dot(comb, gback[...])).astype(BF16)

    settle(gg_ref, v_sum.at[0], pl.ds(0, n))
    for f in range(tiles - 2, tiles):
        put1(f, f % 2).wait()
        put2(f, f % 2).wait()
    each_partner(everyone, lambda q, d: one_row(rows_s, rows_r, d, s_row, v_row, q, d).wait_send())
    each_partner(everyone, lambda q, d: one_row(dots_s, dots_r, q, s_dot, v_dot, q, d).wait_send())
    each_partner(everyone, lambda q, d: one_row(part_s, part_r, d, s_part, v_part, q, d).wait_send())
    each_partner(everyone, lambda q, d: one_row(sum_s, gg_ref, 0, s_sum, v_sum, q, d).wait_send())
    for ref, sem in ((sx, s_x), (sr, s_r), (gs, s_g)):
        settle(ref, sem.at[0], pl.ds(rows, half - rows))
        settle(ref, sem.at[1], half_at(1))


def solution(mesh):
    n = mesh.shape['ep']

    def layer_body(x_loc, r_loc, w_gate, w_in_loc, w_out_loc, first_ids, second_ids, keep_ids):
        groups, seq, hidden = x_loc.shape
        cap = 2 * seq // w_gate.shape[1]
        ff = w_in_loc.shape[2]
        tokens = groups * seq
        slots = n * groups * cap
        tile = 512
        ids = jnp.concatenate([first_ids.reshape(1, tokens), second_ids.reshape(1, tokens), keep_ids.reshape(1, tokens), jnp.zeros((5, tokens), jnp.int32)])
        vmem = pl.BlockSpec(memory_space=pltpu.VMEM)
        hbm = pl.BlockSpec(memory_space=pl.ANY)
        dma = pltpu.SemaphoreType.DMA
        out = pl.pallas_call(
            functools.partial(layer_kernel, n, cap, seq),
            name='moe_layer',
            out_shape=(
                jax.ShapeDtypeStruct((8, 128), F32),
                jax.ShapeDtypeStruct((tokens, hidden), BF16),
                jax.ShapeDtypeStruct((n, hidden), F32),
                jax.ShapeDtypeStruct((hidden, ff), BF16),
                jax.ShapeDtypeStruct((ff, hidden), BF16),
            ),
            in_specs=[vmem, vmem, vmem, vmem, hbm, hbm],
            out_specs=(vmem, vmem, vmem, hbm, hbm),
            scratch_shapes=[
                pltpu.VMEM((hidden, ff), BF16),
                pltpu.VMEM((ff, hidden), BF16),
                pltpu.VMEM((slots, hidden), BF16),
                pltpu.VMEM((slots, hidden), BF16),
                pltpu.VMEM((slots, hidden), BF16),
                pltpu.VMEM((slots, hidden), BF16),
                pltpu.VMEM((slots, hidden), BF16),
                pltpu.VMEM((slots, ff), BF16),
                pltpu.VMEM((slots, ff), BF16),
                pltpu.VMEM((slots, hidden), BF16),
                pltpu.VMEM((slots, hidden), BF16),
                pltpu.VMEM((n, 128), F32),
                pltpu.VMEM((n, 128), F32),
                pltpu.VMEM((n, 128), F32),
                pltpu.VMEM((n, 128), F32),
                pltpu.VMEM((n, hidden), F32),
                pltpu.VMEM((n, hidden), F32),
                pltpu.VMEM((8, hidden), F32),
                pltpu.VMEM((slots // 2, hidden), F32),
                pltpu.VMEM((slots // 2, hidden), F32),
                pltpu.VMEM((hidden, slots), BF16),
                pltpu.VMEM((2, hidden, tile), BF16),
                pltpu.VMEM((2, tile, hidden), BF16),
                dma((2,)), dma((4,)),
                dma((2,)), dma((2,)), dma((2,)), dma((n,)), dma((n,)), dma((n,)), dma((n,)),
                dma((2,)), dma((2,)), dma((2,)), dma((1,)), dma((1,)), dma((1,)), dma((1,)),
            ],
            compiler_params=pltpu.CompilerParams(collective_id=0, has_side_effects=True, vmem_limit_bytes=60 * 1024 * 1024),
        )(ids, x_loc.reshape(tokens, hidden), r_loc.reshape(tokens, hidden), w_gate.T, w_in_loc[0], w_out_loc[0])
        loss, gx, gg, gw1, gw2 = out
        return loss[0, 0], gx.reshape(x_loc.shape), gw1[None], gw2[None], gg.T

    row_spec = P('ep', None, None)
    id_spec = P('ep', None)
    return jax.shard_map(layer_body, mesh=mesh, in_specs=(row_spec, row_spec, P(None, None), row_spec, row_spec, id_spec, id_spec, id_spec), out_specs=(P(), row_spec, row_spec, row_spec, P(None, None)), check_vma=False)
```

```python
import functools

import jax
import jax.numpy as jnp
from jax import lax
from jax.experimental import pallas as pl
from jax.experimental.pallas import tpu as pltpu
from jax.sharding import PartitionSpec as P

ALPHA = 0.01
MESH = pl.DeviceIdType.MESH
F32 = jnp.float32
BF16 = jnp.bfloat16
NN = (((1,), (0,)), ((), ()))
NT = (((1,), (1,)), ((), ()))
TN = (((0,), (0,)), ((), ()))
GELU_C = 0.7978845608028654
GELU_K = 0.044715


def dot(a, b, dims=NN, **kw):
    return lax.dot_general(a, b, dims, preferred_element_type=F32, **kw)


def iota(shape, dim):
    return lax.broadcasted_iota(jnp.int32, shape, dim)


def flip_bits(a, b):
    return a + b - 2 * a * b


def layer_kernel(n, cap, seq, e1_ref, e2_ref, k2_ref, x_ref, r_ref, wg_ref, w1_hbm, w2_hbm,
                 loss_ref, gx_ref, gg_ref, gw1, gw2,
                 w1, w2, sx, sr, xe, re, gy, act, gpre, gs, gback, rows_s, rows_r, dots_s, dots_r,
                 part_s, part_r, sum_s, acc, slope, hid, xet,
                 w_sem, s_x, s_r, s_g, s_row, s_dot, s_part, s_sum,
                 v_x, v_r, v_g, v_row, v_dot, v_part, v_sum):
    me = lax.axis_index('ep')
    tokens, hidden = x_ref.shape
    ff = w1.shape[1]
    groups = tokens // seq
    rows = groups * cap
    slots = n * rows
    half = slots // 2
    plane = n // 4
    tokens_all = tokens * n
    numel = tokens_all * hidden
    tile = 512
    tiles = ff // tile

    low, high = lax.rem(me, plane), lax.div(me, plane)
    low_bits = [lax.rem(low, 2), lax.rem(lax.div(low, 2), 2), lax.div(low, 4)]
    high_bits = [lax.rem(high, 2), lax.div(high, 2)]
    order = (0, 2, 1, 3)

    def partner(quarter, step):
        far = order[quarter]
        top = [bit if not (far >> i) & 1 else 1 - bit for i, bit in enumerate(high_bits)]
        step_bits = [lax.rem(step, 2), lax.rem(lax.div(step, 2), 2), lax.div(step, 4)]
        bits = [flip_bits(a, b) for a, b in zip(low_bits, step_bits)]
        return (top[0] + 2 * top[1]) * plane + bits[0] + 2 * bits[1] + 4 * bits[2]

    def each_partner(quarters, body):
        for quarter in quarters:
            first = 1 if quarter == 0 else 0

            @pl.loop(first, plane)
            def _(step):
                body(quarter * plane + step, partner(quarter, step))

    everyone = (0, 1, 2, 3)
    quarters_of = ((0, 1), (2, 3))

    barrier = pltpu.get_barrier_semaphore()
    each_partner(everyone, lambda q, d: pl.semaphore_signal(barrier, inc=1, device_id=(d,), device_id_type=MESH))
    w1_copy = pltpu.make_async_copy(w1_hbm, w1, w_sem.at[0])
    w2_copy = pltpu.make_async_copy(w2_hbm, w2, w_sem.at[1])
    w1_copy.start()
    w2_copy.start()

    spread = (iota((seq, tokens), 1) % seq == iota((seq, tokens), 0)).astype(F32).astype(BF16)
    own_group = iota((groups, tokens), 1) // seq == iota((groups, tokens), 0)

    def along_lanes(ref):
        wide = dot(ref[...].astype(F32).astype(BF16), spread)
        return jnp.sum(jnp.where(own_group, wide, 0.0), axis=0, keepdims=True).astype(jnp.int32)

    e1, e2, k2 = along_lanes(e1_ref), along_lanes(e2_ref), along_lanes(k2_ref)
    row_i, col_i = iota((tokens, tokens), 0), iota((tokens, tokens), 1)
    eye = row_i == col_i

    def column(row):
        return jnp.sum(jnp.where(eye, row, 0), axis=1, keepdims=True)

    e1c, e2c, k2c = column(e1), column(e2), column(k2)
    same_group = (row_i // seq) == (col_i // seq)
    earlier = same_group & (row_i < col_i)
    one = jnp.int32(1)
    pos1 = jnp.sum(jnp.where(earlier & (e1c == e1), one, 0), axis=0, keepdims=True)
    count1 = jnp.sum(jnp.where(same_group & (e1c == e2), one, 0), axis=0, keepdims=True)
    before2 = jnp.sum(jnp.where(earlier & (e2c == e2) & (k2c > 0), one, 0), axis=0, keepdims=True)
    pos2 = count1 + before2
    lane = iota((1, tokens), 1)
    group_base = (lane // seq) * cap
    kept1 = pos1 < cap
    kept2 = (pos2 < cap) & (k2 > 0)
    place1 = jnp.where(kept1, group_base + pos1, -1)
    place2 = jnp.where(kept2, group_base + pos2, -1)

    def slot_of(expert):
        apart = expert ^ me
        top = apart // plane
        swapped = (top // 2) + 2 * (top % 2)
        return swapped * plane + apart % plane

    key1 = jnp.where(kept1, slot_of(e1) * rows + place1, -1)
    key2 = jnp.where(kept2, slot_of(e2) * rows + place2, -1)
    slot_i = iota((slots, tokens), 0)
    disp = ((slot_i == key1) | (slot_i == key2)).astype(F32).astype(BF16)

    x = x_ref[...]
    sx[...] = dot(disp, x).astype(BF16)

    pl.semaphore_wait(barrier, n - 1)

    def one_row(src, dst, src_row, send, recv, q, d):
        return pltpu.make_async_remote_copy(src.at[pl.ds(src_row, 1)], dst.at[pl.ds(me, 1)], send.at[q], recv.at[0], device_id=(d,), device_id_type=MESH)

    def block(src, dst, send, recv, half_i, q, d):
        at = pl.ds(q * rows, rows)
        return pltpu.make_async_remote_copy(src.at[at], dst.at[at], send.at[half_i], recv.at[half_i], device_id=(d,), device_id_type=MESH)

    def own_row(src, dst, src_row, recv):
        pltpu.make_async_copy(src.at[pl.ds(src_row, 1)], dst.at[pl.ds(me, 1)], recv.at[0]).start()

    def own_block(src, dst, recv):
        pltpu.make_async_copy(src.at[pl.ds(0, rows)], dst.at[pl.ds(0, rows)], recv.at[0]).start()

    def settle(ref, sem, rows_at):
        pltpu.make_async_copy(ref.at[rows_at], ref.at[rows_at], sem).wait()

    def half_at(c):
        return pl.ds(c * half, half)

    for c in range(2):
        each_partner(quarters_of[c], lambda q, d: block(sx, xe, s_x, v_x, c, q, d).start())
    own_block(sx, xe, v_x)

    expert_i = iota((n, tokens), 0)
    hot1 = (expert_i == e1).astype(F32)
    hot2 = (expert_i == e2).astype(F32)
    place_i = iota((128, tokens), 0)
    at1 = (place_i == place1).astype(F32)
    at2 = (place_i == place2).astype(F32)

    wgt = wg_ref[...]
    logits = dot(wgt, x, NT)
    top_logit = jnp.max(logits, axis=0, keepdims=True)
    expd = jnp.exp(logits - top_logit)
    prob = expd / jnp.sum(expd, axis=0, keepdims=True)
    g1 = jnp.sum(prob * hot1, axis=0, keepdims=True)
    g2 = jnp.sum(prob * hot2, axis=0, keepdims=True)
    gsum = g1 + g2
    n1 = (g1 / gsum).astype(BF16).astype(F32)
    n2 = (g2 / gsum).astype(BF16).astype(F32)
    norm_rows = dot((hot1 * n1).astype(BF16), at1.astype(BF16), NT) + dot((hot2 * n2).astype(BF16), at2.astype(BF16), NT)
    sub_n, lane_n = iota((n, 128), 0), iota((n, 128), 1)

    def as_lanes(col, base):
        return jnp.sum(jnp.where(lane_n == sub_n + base, col, 0.0), axis=0, keepdims=True)

    def as_column(row, base):
        return jnp.sum(jnp.where(lane_n == sub_n + base, row, 0.0), axis=1, keepdims=True)

    r = r_ref[...]
    xr = jnp.sum(jnp.sum(x.astype(F32) * r.astype(F32), axis=0, keepdims=True), axis=1, keepdims=True)
    lane_1 = iota((1, 128), 1)
    stats = as_lanes(jnp.sum(hot1, axis=1, keepdims=True), 32) + as_lanes(jnp.sum(prob, axis=1, keepdims=True), 64) + jnp.where(lane_1 == 96, xr, 0.0)
    rows_s[...] = norm_rows + stats

    sr[...] = dot(disp, r).astype(BF16)
    each_partner(everyone, lambda q, d: one_row(rows_s, rows_r, d, s_row, v_row, q, d).start())
    own_row(rows_s, rows_r, me, v_row)
    for c in range(2):
        each_partner(quarters_of[c], lambda q, d: block(sr, re, s_r, v_r, c, q, d).start())
    own_block(sr, re, v_r)

    w1_copy.wait()
    w2_copy.wait()
    for c in range(2):
        at = half_at(c)
        settle(xe, v_x.at[c], at)
        acc[...] = jnp.zeros_like(acc)

        @pl.loop(0, tiles)
        def _(f):
            cols = pl.ds(pl.multiple_of(f * tile, tile), tile)
            pre = dot(xe[at, :], w1[:, cols])
            sq = pre * pre
            th = jnp.tanh(GELU_C * (pre + GELU_K * (sq * pre)))
            cdf = 0.5 * (1.0 + th)
            a = (pre * cdf).astype(BF16)
            slope[at, cols] = cdf + (0.5 * GELU_C) * pre * (1.0 - th * th) * (1.0 + 3 * GELU_K * sq)
            act[at, cols] = a
            acc[...] += dot(a, w2[cols, :])

        hid[at, :] = acc[...].astype(BF16)

    xet[...] = jnp.transpose(xe[...])

    settle(rows_r, v_row.at[0], pl.ds(0, n))
    all_rows = rows_r[...]
    total = jnp.sum(all_rows, axis=0, keepdims=True)
    frac = as_column(total, 32) / tokens_all
    mean_prob = as_column(total, 64) / tokens_all

    loss_part = jnp.zeros((1, 1), F32)
    for c in range(2):
        at = half_at(c)
        slot_row = iota((half, n), 0) + c * half
        apart = slot_row // rows
        top = apart // plane
        source = (((top // 2) + 2 * (top % 2)) * plane + apart % plane) ^ me
        pick = (source == iota((half, n), 1)).astype(F32).astype(BF16)
        wide = dot(pick, all_rows.astype(BF16))
        mine = iota((half, 128), 1) == iota((half, 128), 0) % rows
        norm = jnp.sum(jnp.where(mine, wide, 0.0), axis=1, keepdims=True)
        settle(re, v_r.at[c], at)
        rc = re[at, :].astype(F32)
        gy[at, :] = (norm * rc).astype(BF16)
        d = jnp.sum(hid[at, :].astype(F32) * rc, axis=1, keepdims=True)
        loss_part = loss_part + jnp.sum(norm * d, axis=0, keepdims=True)
        in_lane = jnp.where(mine, d, 0.0)
        dots_s[pl.ds(c * (n // 2), n // 2), :] = jnp.sum(in_lane.reshape(n // 2, rows, 128), axis=1)
        if c == 1:
            dots_s[...] = dots_s[...] + jnp.where(lane_1 == 16, loss_part, 0.0)
            each_partner(everyone, lambda q, d: one_row(dots_s, dots_r, q, s_dot, v_dot, q, d).start())
            own_row(dots_s, dots_r, 0, v_dot)
        acc[...] = jnp.zeros_like(acc)

        @pl.loop(0, tiles)
        def _(f):
            cols = pl.ds(pl.multiple_of(f * tile, tile), tile)
            ga = dot(gy[at, :], w2[cols, :], NT).astype(BF16)
            gp = (ga.astype(F32) * slope[at, cols]).astype(BF16)
            gpre[at, cols] = gp
            acc[...] += dot(gp, w1[:, cols], NT)

        gs[at, :] = acc[...].astype(BF16)
        if c == 0:
            own_block(gs, gback, v_g)
        each_partner(quarters_of[c], lambda q, d: block(gs, gback, s_g, v_g, c, q, d).start())

    @pl.loop(0, tiles)
    def _(f):
        cols = pl.ds(pl.multiple_of(f * tile, tile), tile)
        gw1[:, cols] = dot(xet[...], gpre[:, cols]).astype(BF16)

    settle(dots_r, v_dot.at[0], pl.ds(0, n))
    all_dots = dots_r[...]
    exact = lax.Precision.HIGHEST
    d1 = jnp.sum(dot(all_dots, hot1, TN, precision=exact) * at1, axis=0, keepdims=True)
    d2 = jnp.sum(dot(all_dots, hot2, TN, precision=exact) * at2, axis=0, keepdims=True)
    d1 = d1.astype(BF16).astype(F32)
    d2 = d2.astype(BF16).astype(F32)
    gate_sq = gsum * gsum
    up1 = (d1 - d2) * g2 / gate_sq
    up2 = (d2 - d1) * g1 / gate_sq
    gprob = up1 * hot1 + up2 * hot2 + (ALPHA * hidden * n) * frac
    glog = (prob * (gprob - jnp.sum(prob * gprob, axis=0, keepdims=True))).astype(BF16)
    part_s[...] = dot(glog, x)
    each_partner(everyone, lambda q, d: one_row(part_s, part_r, d, s_part, v_part, q, d).start())
    own_row(part_s, part_r, me, v_part)

    both = jnp.sum(jnp.where(lane_1 == 96, total, 0.0), axis=1, keepdims=True)
    both = both + jnp.sum(jnp.where(lane_1 == 16, jnp.sum(all_dots, axis=0, keepdims=True), 0.0), axis=1, keepdims=True)
    aux = jnp.sum(frac * mean_prob, axis=0, keepdims=True) * n
    loss_ref[...] = jnp.broadcast_to(both / numel + ALPHA * aux, loss_ref.shape)

    @pl.loop(0, tiles)
    def _(f):
        cols = pl.ds(pl.multiple_of(f * tile, tile), tile)
        gw2[cols, :] = dot(act[:, cols], gy[...], TN).astype(BF16)

    settle(part_r, v_part.at[0], pl.ds(0, n))
    sum_s[0:1, :] = jnp.sum(part_r[...], axis=0, keepdims=True)
    each_partner(everyone, lambda q, d: one_row(sum_s, gg_ref, 0, s_sum, v_sum, q, d).start())
    own_row(sum_s, gg_ref, 0, v_sum)

    key1c, key2c = column(key1), column(key2)
    slot_l = iota((tokens, slots), 1)
    comb = ((slot_l == key1c) | (slot_l == key2c)).astype(F32).astype(BF16)
    near = r.astype(F32) + dot(glog, wgt, TN)
    for c in range(2):
        settle(gback, v_g.at[c], half_at(c))
    gx_ref[...] = (near + dot(comb, gback[...])).astype(BF16)

    settle(gg_ref, v_sum.at[0], pl.ds(0, n))
    each_partner(everyone, lambda q, d: one_row(rows_s, rows_r, d, s_row, v_row, q, d).wait_send())
    each_partner(everyone, lambda q, d: one_row(dots_s, dots_r, q, s_dot, v_dot, q, d).wait_send())
    each_partner(everyone, lambda q, d: one_row(part_s, part_r, d, s_part, v_part, q, d).wait_send())
    each_partner(everyone, lambda q, d: one_row(sum_s, gg_ref, 0, s_sum, v_sum, q, d).wait_send())
    for ref, sem in ((sx, s_x), (sr, s_r), (gs, s_g)):
        settle(ref, sem.at[0], pl.ds(rows, half - rows))
        settle(ref, sem.at[1], half_at(1))


def solution(mesh):
    n = mesh.shape['ep']

    def layer_body(x_loc, r_loc, w_gate, w_in_loc, w_out_loc, first_ids, second_ids, keep_ids):
        groups, seq, hidden = x_loc.shape
        cap = 2 * seq // w_gate.shape[1]
        ff = w_in_loc.shape[2]
        tokens = groups * seq
        slots = n * groups * cap
        vmem = pl.BlockSpec(memory_space=pltpu.VMEM)
        hbm = pl.BlockSpec(memory_space=pl.ANY)
        dma = pltpu.SemaphoreType.DMA
        out = pl.pallas_call(
            functools.partial(layer_kernel, n, cap, seq),
            name='moe_layer',
            out_shape=(
                pltpu.VMEM((8, 128), F32),
                pltpu.VMEM((tokens, hidden), BF16),
                pltpu.VMEM((n, hidden), F32),
                pltpu.VMEM((hidden, ff), BF16),
                pltpu.VMEM((ff, hidden), BF16),
            ),
            in_specs=[vmem] * 6 + [hbm, hbm],
            out_specs=(vmem,) * 5,
            scratch_shapes=[
                pltpu.VMEM((hidden, ff), BF16),
                pltpu.VMEM((ff, hidden), BF16),
                pltpu.VMEM((slots, hidden), BF16),
                pltpu.VMEM((slots, hidden), BF16),
                pltpu.VMEM((slots, hidden), BF16),
                pltpu.VMEM((slots, hidden), BF16),
                pltpu.VMEM((slots, hidden), BF16),
                pltpu.VMEM((slots, ff), BF16),
                pltpu.VMEM((slots, ff), BF16),
                pltpu.VMEM((slots, hidden), BF16),
                pltpu.VMEM((slots, hidden), BF16),
                pltpu.VMEM((n, 128), F32),
                pltpu.VMEM((n, 128), F32),
                pltpu.VMEM((n, 128), F32),
                pltpu.VMEM((n, 128), F32),
                pltpu.VMEM((n, hidden), F32),
                pltpu.VMEM((n, hidden), F32),
                pltpu.VMEM((8, hidden), F32),
                pltpu.VMEM((slots // 2, hidden), F32),
                pltpu.VMEM((slots, ff), F32),
                pltpu.VMEM((slots, hidden), BF16),
                pltpu.VMEM((hidden, slots), BF16),
                dma((2,)),
                dma((2,)), dma((2,)), dma((2,)), dma((n,)), dma((n,)), dma((n,)), dma((n,)),
                dma((2,)), dma((2,)), dma((2,)), dma((1,)), dma((1,)), dma((1,)), dma((1,)),
            ],
            compiler_params=pltpu.CompilerParams(collective_id=0, has_side_effects=True, vmem_limit_bytes=44 * 1024 * 1024),
        )(first_ids, second_ids, keep_ids, x_loc.reshape(tokens, hidden), r_loc.reshape(tokens, hidden), w_gate.T, w_in_loc[0], w_out_loc[0])
        loss, gx, gg, gw1, gw2 = out
        return loss[0, 0], gx.reshape(x_loc.shape), gw1[None], gw2[None], gg.T

    row_spec = P('ep', None, None)
    id_spec = P('ep', None)
    return jax.shard_map(layer_body, mesh=mesh, in_specs=(row_spec, row_spec, P(None, None), row_spec, row_spec, id_spec, id_spec, id_spec), out_specs=(P(), row_spec, row_spec, row_spec, P(None, None)), check_vma=False)
```

```python
import functools

import jax
import jax.numpy as jnp
from jax import lax
from jax.experimental import pallas as pl
from jax.experimental.pallas import tpu as pltpu
from jax.sharding import PartitionSpec as P

ALPHA = 0.01
MESH = pl.DeviceIdType.MESH
F32 = jnp.float32
BF16 = jnp.bfloat16
NN = (((1,), (0,)), ((), ()))
NT = (((1,), (1,)), ((), ()))
TN = (((0,), (0,)), ((), ()))
GELU_C = 0.7978845608028654
GELU_K = 0.044715


def dot(a, b, dims=NN, **kw):
    return lax.dot_general(a, b, dims, preferred_element_type=F32, **kw)


def iota(shape, dim):
    return lax.broadcasted_iota(jnp.int32, shape, dim)


def flip_bits(a, b):
    return a + b - 2 * a * b


def write_kernel(loss_v, gx_v, gg_v, gw1_v, gw2_v, loss_s, gx_h, gg_h, gw1_h, gw2_h, sem):
    copies = [pltpu.make_async_copy(src, dst, sem.at[i]) for i, (src, dst) in enumerate(((gw1_v, gw1_h), (gw2_v, gw2_h), (gx_v, gx_h), (gg_v, gg_h)))]
    for copy in copies:
        copy.start()
    loss_s[0, 0] = jnp.max(loss_v[...])
    for copy in copies:
        copy.wait()


def layer_kernel(n, cap, seq, e1_hbm, e2_hbm, k2_hbm, x_hbm, r_hbm, wg_hbm, w1_hbm, w2_hbm,
                 loss_ref, gx_ref, gg_ref, gw1, gw2,
                 e1_ref, e2_ref, k2_ref, x_ref, r_ref, wg_ref, w1, w2, sx, sr, xe, re, gy, act, gpre, gs, gback,
                 rows_s, rows_r, dots_s, dots_r, part_s, part_r, sum_s, acc, slope, hid, xet, in_sem,
                 s_x, s_r, s_g, s_row, s_dot, s_part, s_sum,
                 v_x, v_r, v_g, v_row, v_dot, v_part, v_sum):
    me = lax.axis_index('ep')
    tokens, hidden = x_ref.shape
    ff = w1.shape[1]
    groups = tokens // seq
    rows = groups * cap
    slots = n * rows
    plane = n // 4
    tokens_all = tokens * n
    numel = tokens_all * hidden
    tile = 512
    tiles = ff // tile

    low, high = lax.rem(me, plane), lax.div(me, plane)
    low_bits = [lax.rem(low, 2), lax.rem(lax.div(low, 2), 2), lax.div(low, 4)]
    high_bits = [lax.rem(high, 2), lax.div(high, 2)]
    order = (2, 0, 1, 3)
    own = plane * rows

    def partner(quarter, step):
        far = order[quarter]
        top = [bit if not (far >> i) & 1 else 1 - bit for i, bit in enumerate(high_bits)]
        step_bits = [lax.rem(step, 2), lax.rem(lax.div(step, 2), 2), lax.div(step, 4)]
        bits = [flip_bits(a, b) for a, b in zip(low_bits, step_bits)]
        return (top[0] + 2 * top[1]) * plane + bits[0] + 2 * bits[1] + 4 * bits[2]

    def each_partner(pieces, body):
        for quarter, lo, hi in pieces:
            first = max(lo, 1) if order[quarter] == 0 else lo

            @pl.loop(first, hi)
            def _(step):
                body(quarter * plane + step, partner(quarter, step))

    everyone = tuple((quarter, 0, plane) for quarter in (0, 3, 1, 2))
    early, near, late = 0, 1, 2
    quarters_of = (((0, 0, plane),), ((1, 0, plane), (2, 0, plane)), ((3, 0, plane),))
    span = ((0, plane * rows), (plane * rows, 2 * plane * rows), (3 * plane * rows, plane * rows))

    barrier = pltpu.get_barrier_semaphore()
    each_partner(everyone, lambda q, d: pl.semaphore_signal(barrier, inc=1, device_id=(d,), device_id_type=MESH))
    fetched = [pltpu.make_async_copy(src, dst, in_sem.at[i]) for i, (src, dst) in enumerate((
        (e1_hbm, e1_ref), (e2_hbm, e2_ref), (k2_hbm, k2_ref), (x_hbm, x_ref), (r_hbm, r_ref), (wg_hbm, wg_ref), (w1_hbm, w1), (w2_hbm, w2)))]
    for copy in fetched:
        copy.start()
    for copy in fetched[:3]:
        copy.wait()

    spread = (iota((seq, tokens), 1) % seq == iota((seq, tokens), 0)).astype(F32).astype(BF16)
    own_group = iota((groups, tokens), 1) // seq == iota((groups, tokens), 0)

    def along_lanes(ref):
        wide = dot(ref[...].astype(F32).astype(BF16), spread)
        return jnp.sum(jnp.where(own_group, wide, 0.0), axis=0, keepdims=True).astype(jnp.int32)

    e1, e2, k2 = along_lanes(e1_ref), along_lanes(e2_ref), along_lanes(k2_ref)
    row_i, col_i = iota((tokens, tokens), 0), iota((tokens, tokens), 1)
    eye = row_i == col_i

    def column(row):
        return jnp.sum(jnp.where(eye, row, 0), axis=1, keepdims=True)

    e1c, e2c, k2c = column(e1), column(e2), column(k2)
    same_group = (row_i // seq) == (col_i // seq)
    earlier = same_group & (row_i < col_i)
    one = jnp.int32(1)
    pos1 = jnp.sum(jnp.where(earlier & (e1c == e1), one, 0), axis=0, keepdims=True)
    count1 = jnp.sum(jnp.where(same_group & (e1c == e2), one, 0), axis=0, keepdims=True)
    before2 = jnp.sum(jnp.where(earlier & (e2c == e2) & (k2c > 0), one, 0), axis=0, keepdims=True)
    pos2 = count1 + before2
    lane = iota((1, tokens), 1)
    group_base = (lane // seq) * cap
    kept1 = pos1 < cap
    kept2 = (pos2 < cap) & (k2 > 0)
    place1 = jnp.where(kept1, group_base + pos1, -1)
    place2 = jnp.where(kept2, group_base + pos2, -1)

    def slot_of(expert):
        apart = expert ^ me
        top = apart // plane
        quarter = jnp.where(top == order[0], 0, jnp.where(top == order[3], 3, top + 1))
        return quarter * plane + apart % plane

    key1 = jnp.where(kept1, slot_of(e1) * rows + place1, -1)
    key2 = jnp.where(kept2, slot_of(e2) * rows + place2, -1)
    slot_i = iota((slots, tokens), 0)
    disp = ((slot_i == key1) | (slot_i == key2)).astype(F32).astype(BF16)

    fetched[3].wait()
    x = x_ref[...]
    sx[...] = dot(disp, x).astype(BF16)

    pl.semaphore_wait(barrier, n - 1)

    def one_row(src, dst, src_row, send, recv, q, d):
        return pltpu.make_async_remote_copy(src.at[pl.ds(src_row, 1)], dst.at[pl.ds(me, 1)], send.at[q], recv.at[0], device_id=(d,), device_id_type=MESH)

    def block(src, dst, send, recv, half_i, q, d):
        at = pl.ds(q * rows, rows)
        return pltpu.make_async_remote_copy(src.at[at], dst.at[at], send.at[half_i], recv.at[half_i], device_id=(d,), device_id_type=MESH)

    def own_row(src, dst, src_row, recv):
        pltpu.make_async_copy(src.at[pl.ds(src_row, 1)], dst.at[pl.ds(me, 1)], recv.at[0]).start()

    def own_block(src, dst, recv):
        pltpu.make_async_copy(src.at[pl.ds(own, rows)], dst.at[pl.ds(own, rows)], recv.at[near]).start()

    def settle(ref, sem, rows_at):
        pltpu.make_async_copy(ref.at[rows_at], ref.at[rows_at], sem).wait()

    def group_at(c):
        return pl.ds(*span[c])

    def send_group(src, dst, send, recv, c, pieces=None):
        each_partner(pieces or quarters_of[c], lambda q, d: block(src, dst, send, recv, c, q, d).start())

    send_group(sx, xe, s_x, v_x, early)
    send_group(sx, xe, s_x, v_x, near)
    own_block(sx, xe, v_x)
    fetched[4].wait()
    fetched[5].wait()

    expert_i = iota((n, tokens), 0)
    hot1 = (expert_i == e1).astype(F32)
    hot2 = (expert_i == e2).astype(F32)
    place_i = iota((128, tokens), 0)
    at1 = (place_i == place1).astype(F32)
    at2 = (place_i == place2).astype(F32)

    wgt = wg_ref[...]
    logits = dot(wgt, x, NT)
    top_logit = jnp.max(logits, axis=0, keepdims=True)
    expd = jnp.exp(logits - top_logit)
    prob = expd / jnp.sum(expd, axis=0, keepdims=True)
    g1 = jnp.sum(prob * hot1, axis=0, keepdims=True)
    g2 = jnp.sum(prob * hot2, axis=0, keepdims=True)
    gsum = g1 + g2
    n1 = (g1 / gsum).astype(BF16).astype(F32)
    n2 = (g2 / gsum).astype(BF16).astype(F32)
    norm_rows = dot((hot1 * n1).astype(BF16), at1.astype(BF16), NT) + dot((hot2 * n2).astype(BF16), at2.astype(BF16), NT)
    sub_n, lane_n = iota((n, 128), 0), iota((n, 128), 1)

    def as_lanes(col, base):
        return jnp.sum(jnp.where(lane_n == sub_n + base, col, 0.0), axis=0, keepdims=True)

    def as_column(row, base):
        return jnp.sum(jnp.where(lane_n == sub_n + base, row, 0.0), axis=1, keepdims=True)

    r = r_ref[...]
    xr = jnp.sum(jnp.sum(x.astype(F32) * r.astype(F32), axis=0, keepdims=True), axis=1, keepdims=True)
    lane_1 = iota((1, 128), 1)
    stats = as_lanes(jnp.sum(hot1, axis=1, keepdims=True), 32) + as_lanes(jnp.sum(prob, axis=1, keepdims=True), 64) + jnp.where(lane_1 == 96, xr, 0.0)
    rows_s[...] = norm_rows + stats

    sr[...] = dot(disp, r).astype(BF16)
    each_partner(everyone, lambda q, d: one_row(rows_s, rows_r, d, s_row, v_row, q, d).start())
    own_row(rows_s, rows_r, me, v_row)
    send_group(sr, re, s_r, v_r, early)
    send_group(sx, xe, s_x, v_x, late)
    send_group(sr, re, s_r, v_r, near)
    own_block(sr, re, v_r)
    send_group(sr, re, s_r, v_r, late)

    slot_row = iota((slots, n), 0)
    quarter = slot_row // rows // plane
    far = jnp.where(quarter == 0, order[0], jnp.where(quarter == 3, order[3], quarter - 1))
    source = (far * plane + slot_row // rows % plane) ^ me
    pick = (source == iota((slots, n), 1)).astype(F32).astype(BF16)
    mine = iota((slots, 128), 1) == iota((slots, 128), 0) % rows
    key1c, key2c = column(key1), column(key2)
    slot_l = iota((tokens, slots), 1)
    comb = ((slot_l == key1c) | (slot_l == key2c)).astype(F32).astype(BF16)
    fetched[6].wait()
    fetched[7].wait()

    def forward(c):
        at = group_at(c)
        settle(xe, v_x.at[c], at)
        total_at = pl.ds(0, span[c][1])
        acc[total_at, :] = jnp.zeros((span[c][1], hidden), F32)

        @pl.loop(0, tiles)
        def _(f):
            cols = pl.ds(pl.multiple_of(f * tile, tile), tile)
            pre = dot(xe[at, :], w1[:, cols])
            sq = pre * pre
            th = jnp.tanh(GELU_C * (pre + GELU_K * (sq * pre)))
            cdf = 0.5 * (1.0 + th)
            a = (pre * cdf).astype(BF16)
            slope[at, cols] = cdf + (0.5 * GELU_C) * pre * (1.0 - th * th) * (1.0 + 3 * GELU_K * sq)
            act[at, cols] = a
            acc[total_at, :] += dot(a, w2[cols, :])

        hid[at, :] = acc[total_at, :].astype(BF16)

    def receive(c):
        at = group_at(c)
        start, size = span[c]
        settle(re, v_r.at[c], at)
        rc = re[at, :].astype(F32)
        norm = norms[start:start + size]
        gy[at, :] = (norm * rc).astype(BF16)
        d = jnp.sum(hid[at, :].astype(F32) * rc, axis=1, keepdims=True)
        in_lane = jnp.where(mine[start:start + size], d, 0.0)
        dots_s[pl.ds(start // rows, size // rows), :] = jnp.sum(in_lane.reshape(size // rows, rows, 128), axis=1)
        return jnp.sum(norm * d, axis=0, keepdims=True)

    def backward(c):
        at = group_at(c)
        total_at = pl.ds(0, span[c][1])
        acc[total_at, :] = jnp.zeros((span[c][1], hidden), F32)

        @pl.loop(0, tiles)
        def _(f):
            cols = pl.ds(pl.multiple_of(f * tile, tile), tile)
            ga = dot(gy[at, :], w2[cols, :], NT).astype(BF16)
            gp = (ga.astype(F32) * slope[at, cols]).astype(BF16)
            gpre[at, cols] = gp
            acc[total_at, :] += dot(gp, w1[:, cols], NT)

        gs[at, :] = acc[total_at, :].astype(BF16)

    def send_back(c, pieces=None):
        send_group(gs, gback, s_g, v_g, c, pieces)

    def grad_first(lo, hi):
        @pl.loop(lo, hi)
        def _(f):
            cols = pl.ds(pl.multiple_of(f * tile, tile), tile)
            gw1[:, cols] = dot(xet[...], gpre[:, cols]).astype(BF16)

    def grad_second(lo, hi):
        @pl.loop(lo, hi)
        def _(f):
            cols = pl.ds(pl.multiple_of(f * tile, tile), tile)
            gw2[cols, :] = dot(act[:, cols], gy[...], TN).astype(BF16)

    forward(early)
    forward(near)
    settle(rows_r, v_row.at[0], pl.ds(0, n))
    all_rows = rows_r[...]
    total = jnp.sum(all_rows, axis=0, keepdims=True)
    frac = as_column(total, 32) / tokens_all
    mean_prob = as_column(total, 64) / tokens_all
    norms = jnp.sum(jnp.where(mine, dot(pick, all_rows.astype(BF16)), 0.0), axis=1, keepdims=True)

    loss_part = receive(early)
    backward(early)
    split_early, split_late = 5, 2
    send_back(early, ((0, 0, split_early),))
    loss_part = loss_part + receive(near)
    backward(near)
    send_back(near)
    own_block(gs, gback, v_g)
    forward(late)
    xet[...] = jnp.transpose(xe[...])
    loss_part = loss_part + receive(late)
    dots_s[...] = dots_s[...] + jnp.where(lane_1 == 16, loss_part, 0.0)
    each_partner(everyone, lambda q, d: one_row(dots_s, dots_r, q, s_dot, v_dot, q, d).start())
    own_row(dots_s, dots_r, plane, v_dot)
    send_back(early, ((0, split_early, plane),))
    backward(late)
    send_back(late, ((3, 0, split_late),))
    grad_first(0, 2)

    settle(dots_r, v_dot.at[0], pl.ds(0, n))
    all_dots = dots_r[...]
    exact = lax.Precision.HIGHEST
    d1 = jnp.sum(dot(all_dots, hot1, TN, precision=exact) * at1, axis=0, keepdims=True)
    d2 = jnp.sum(dot(all_dots, hot2, TN, precision=exact) * at2, axis=0, keepdims=True)
    d1 = d1.astype(BF16).astype(F32)
    d2 = d2.astype(BF16).astype(F32)
    gate_sq = gsum * gsum
    up1 = (d1 - d2) * g2 / gate_sq
    up2 = (d2 - d1) * g1 / gate_sq
    gprob = up1 * hot1 + up2 * hot2 + (ALPHA * hidden * n) * frac
    glog = (prob * (gprob - jnp.sum(prob * gprob, axis=0, keepdims=True))).astype(BF16)
    part_s[...] = dot(glog, x_ref[...])
    each_partner(everyone, lambda q, d: one_row(part_s, part_r, d, s_part, v_part, q, d).start())
    own_row(part_s, part_r, me, v_part)
    send_back(late, ((3, split_late, plane),))
    grad_first(2, tiles)

    both = jnp.sum(jnp.where(lane_1 == 96, total, 0.0), axis=1, keepdims=True)
    both = both + jnp.sum(jnp.where(lane_1 == 16, jnp.sum(all_dots, axis=0, keepdims=True), 0.0), axis=1, keepdims=True)
    aux = jnp.sum(frac * mean_prob, axis=0, keepdims=True) * n
    loss_ref[...] = jnp.broadcast_to(both / numel + ALPHA * aux, loss_ref.shape)
    grad_second(0, 2)

    settle(part_r, v_part.at[0], pl.ds(0, n))
    sum_s[0:1, :] = jnp.sum(part_r[...], axis=0, keepdims=True)
    each_partner(everyone, lambda q, d: one_row(sum_s, gg_ref, 0, s_sum, v_sum, q, d).start())
    own_row(sum_s, gg_ref, 0, v_sum)

    grad_second(2, tiles)

    out = r_ref[...].astype(F32) + dot(glog, wg_ref[...], TN)
    for c in (near, early, late):
        start, size = span[c]
        settle(gback, v_g.at[c], group_at(c))
        out = out + dot(comb[:, start:start + size], gback[group_at(c), :])
    gx_ref[...] = out.astype(BF16)

    settle(gg_ref, v_sum.at[0], pl.ds(0, n))
    each_partner(everyone, lambda q, d: one_row(rows_s, rows_r, d, s_row, v_row, q, d).wait_send())
    each_partner(everyone, lambda q, d: one_row(dots_s, dots_r, q, s_dot, v_dot, q, d).wait_send())
    each_partner(everyone, lambda q, d: one_row(part_s, part_r, d, s_part, v_part, q, d).wait_send())
    each_partner(everyone, lambda q, d: one_row(sum_s, gg_ref, 0, s_sum, v_sum, q, d).wait_send())
    for ref, sem in ((sx, s_x), (sr, s_r), (gs, s_g)):
        settle(ref, sem.at[early], group_at(early))
        settle(ref, sem.at[near], pl.ds(own + rows, span[near][1] - rows))
        settle(ref, sem.at[late], group_at(late))


def solution(mesh):
    n = mesh.shape['ep']

    def layer_body(x_loc, r_loc, w_gate, w_in_loc, w_out_loc, first_ids, second_ids, keep_ids):
        groups, seq, hidden = x_loc.shape
        cap = 2 * seq // w_gate.shape[1]
        ff = w_in_loc.shape[2]
        tokens = groups * seq
        slots = n * groups * cap
        vmem = pl.BlockSpec(memory_space=pltpu.VMEM)
        hbm = pl.BlockSpec(memory_space=pltpu.HBM)
        dma = pltpu.SemaphoreType.DMA
        out = pl.pallas_call(
            functools.partial(layer_kernel, n, cap, seq),
            name='moe_layer',
            out_shape=(
                pltpu.VMEM((8, 128), F32),
                pltpu.VMEM((tokens, hidden), BF16),
                pltpu.VMEM((n, hidden), F32),
                pltpu.VMEM((hidden, ff), BF16),
                pltpu.VMEM((ff, hidden), BF16),
            ),
            in_specs=[hbm] * 8,
            out_specs=(vmem,) * 5,
            scratch_shapes=[
                pltpu.VMEM((groups, seq), jnp.int32),
                pltpu.VMEM((groups, seq), jnp.int32),
                pltpu.VMEM((groups, seq), jnp.int32),
                pltpu.VMEM((tokens, hidden), BF16),
                pltpu.VMEM((tokens, hidden), BF16),
                pltpu.VMEM((n, hidden), BF16),
                pltpu.VMEM((hidden, ff), BF16),
                pltpu.VMEM((ff, hidden), BF16),
                pltpu.VMEM((slots, hidden), BF16),
                pltpu.VMEM((slots, hidden), BF16),
                pltpu.VMEM((slots, hidden), BF16),
                pltpu.VMEM((slots, hidden), BF16),
                pltpu.VMEM((slots, hidden), BF16),
                pltpu.VMEM((slots, ff), BF16),
                pltpu.VMEM((slots, ff), BF16),
                pltpu.VMEM((slots, hidden), BF16),
                pltpu.VMEM((slots, hidden), BF16),
                pltpu.VMEM((n, 128), F32),
                pltpu.VMEM((n, 128), F32),
                pltpu.VMEM((n, 128), F32),
                pltpu.VMEM((n, 128), F32),
                pltpu.VMEM((n, hidden), F32),
                pltpu.VMEM((n, hidden), F32),
                pltpu.VMEM((8, hidden), F32),
                pltpu.VMEM((slots // 2, hidden), F32),
                pltpu.VMEM((slots, ff), F32),
                pltpu.VMEM((slots, hidden), BF16),
                pltpu.VMEM((hidden, slots), BF16),
                dma((8,)),
                dma((3,)), dma((3,)), dma((3,)), dma((n,)), dma((n,)), dma((n,)), dma((n,)),
                dma((3,)), dma((3,)), dma((3,)), dma((1,)), dma((1,)), dma((1,)), dma((1,)),
            ],
            compiler_params=pltpu.CompilerParams(collective_id=0, has_side_effects=True, vmem_limit_bytes=44 * 1024 * 1024),
        )(*(pltpu.with_memory_space_constraint(a, pltpu.HBM) for a in (
            first_ids, second_ids, keep_ids, x_loc.reshape(tokens, hidden), r_loc.reshape(tokens, hidden), w_gate.T, w_in_loc[0], w_out_loc[0])))
        loss, gx, gg, gw1, gw2 = pl.pallas_call(
            write_kernel,
            name='write_results',
            out_shape=(
                jax.ShapeDtypeStruct((1, 1), F32),
                jax.ShapeDtypeStruct((tokens, hidden), BF16),
                jax.ShapeDtypeStruct((n, hidden), F32),
                jax.ShapeDtypeStruct((hidden, ff), BF16),
                jax.ShapeDtypeStruct((ff, hidden), BF16),
            ),
            in_specs=[vmem] * 5,
            out_specs=(pl.BlockSpec(memory_space=pltpu.SMEM), hbm, hbm, hbm, hbm),
            scratch_shapes=[dma((4,))],
            compiler_params=pltpu.CompilerParams(vmem_limit_bytes=2 * 1024 * 1024),
        )(*(pltpu.with_memory_space_constraint(a, pltpu.VMEM) for a in out))
        return loss.reshape(()), gx.reshape(x_loc.shape), gw1[None], gw2[None], gg.T

    row_spec = P('ep', None, None)
    id_spec = P('ep', None)
    return jax.shard_map(layer_body, mesh=mesh, in_specs=(row_spec, row_spec, P(None, None), row_spec, row_spec, id_spec, id_spec, id_spec), out_specs=(P(), row_spec, row_spec, row_spec, P(None, None)), check_vma=False)
```

```python
import functools

import jax
import jax.numpy as jnp
from jax import lax
from jax.experimental import pallas as pl
from jax.experimental.pallas import tpu as pltpu
from jax.sharding import PartitionSpec as P

ALPHA = 0.01
MESH = pl.DeviceIdType.MESH
F32 = jnp.float32
BF16 = jnp.bfloat16
NN = (((1,), (0,)), ((), ()))
NT = (((1,), (1,)), ((), ()))
TN = (((0,), (0,)), ((), ()))
GELU_C = 0.7978845608028654
GELU_K = 0.044715


def dot(a, b, dims=NN, **kw):
    return lax.dot_general(a, b, dims, preferred_element_type=F32, **kw)


def iota(shape, dim):
    return lax.broadcasted_iota(jnp.int32, shape, dim)


def flip_bits(a, b):
    return a + b - 2 * a * b


def write_kernel(loss_v, gx_v, gg_v, gw1_v, gw2_v, loss_s, gx_h, gg_h, gw1_h, gw2_h, sem):
    copies = [pltpu.make_async_copy(src, dst, sem.at[i]) for i, (src, dst) in enumerate(((gw1_v, gw1_h), (gw2_v, gw2_h), (gx_v, gx_h), (gg_v, gg_h)))]
    for copy in copies:
        copy.start()
    loss_s[0, 0] = jnp.max(loss_v[...])
    for copy in copies:
        copy.wait()


def layer_kernel(n, cap, seq, e1_hbm, e2_hbm, k2_hbm, x_hbm, r_hbm, wg_hbm, w1_hbm, w2_hbm,
                 loss_ref, gx_ref, gg_ref, gw1, gw2,
                 e1_ref, e2_ref, k2_ref, x_ref, r_ref, wg_ref, w1, w2, sx, sr, xe, re, gy, act, gpre, gs, gback,
                 rows_s, rows_r, dots_s, dots_r, part_s, part_r, mid_s, mid_r, sum_s, slope, hid, xet, in_sem,
                 s_x, s_r, s_g, s_row, s_dot, s_part, s_mid, s_sum,
                 v_x, v_r, v_g, v_row, v_dot, v_part, v_mid, v_sum):
    me = lax.axis_index('ep')
    tokens, hidden = x_ref.shape
    ff = w1.shape[1]
    groups = tokens // seq
    rows = groups * cap
    slots = n * rows
    plane = n // 4
    tokens_all = tokens * n
    numel = tokens_all * hidden

    low, high = lax.rem(me, plane), lax.div(me, plane)
    low_bits = [lax.rem(low, 2), lax.rem(lax.div(low, 2), 2), lax.div(low, 4)]
    high_bits = [lax.rem(high, 2), lax.div(high, 2)]
    order = (2, 0, 1, 3)
    own = plane * rows

    def partner(quarter, step):
        far = order[quarter]
        top = [bit if not (far >> i) & 1 else 1 - bit for i, bit in enumerate(high_bits)]
        step_bits = [lax.rem(step, 2), lax.rem(lax.div(step, 2), 2), lax.div(step, 4)]
        bits = [flip_bits(a, b) for a, b in zip(low_bits, step_bits)]
        return (top[0] + 2 * top[1]) * plane + bits[0] + 2 * bits[1] + 4 * bits[2]

    def each_partner(pieces, body):
        for quarter, lo, hi in pieces:
            first = max(lo, 1) if order[quarter] == 0 else lo

            @pl.loop(first, hi)
            def _(step):
                body(quarter * plane + step, partner(quarter, step))

    everyone = tuple((quarter, 0, plane) for quarter in (0, 3, 1, 2))
    early, near, late = 0, 1, 2
    quarters_of = (((0, 0, plane),), ((1, 0, plane), (2, 0, plane)), ((3, 0, plane),))
    span = ((0, plane * rows), (plane * rows, 2 * plane * rows), (3 * plane * rows, plane * rows))

    barrier = pltpu.get_barrier_semaphore()
    each_partner(everyone, lambda q, d: pl.semaphore_signal(barrier, inc=1, device_id=(d,), device_id_type=MESH))
    fetched = [pltpu.make_async_copy(src, dst, in_sem.at[i]) for i, (src, dst) in enumerate((
        (e1_hbm, e1_ref), (e2_hbm, e2_ref), (k2_hbm, k2_ref), (x_hbm, x_ref), (r_hbm, r_ref), (wg_hbm, wg_ref), (w1_hbm, w1), (w2_hbm, w2)))]
    for copy in fetched:
        copy.start()
    for copy in fetched[:3]:
        copy.wait()

    spread = (iota((seq, tokens), 1) % seq == iota((seq, tokens), 0)).astype(F32).astype(BF16)
    own_group = iota((groups, tokens), 1) // seq == iota((groups, tokens), 0)

    def along_lanes(ref):
        wide = dot(ref[...].astype(F32).astype(BF16), spread)
        return jnp.sum(jnp.where(own_group, wide, 0.0), axis=0, keepdims=True).astype(jnp.int32)

    e1, e2, k2 = along_lanes(e1_ref), along_lanes(e2_ref), along_lanes(k2_ref)
    row_i, col_i = iota((tokens, tokens), 0), iota((tokens, tokens), 1)
    eye = row_i == col_i

    def column(row):
        return jnp.sum(jnp.where(eye, row, 0), axis=1, keepdims=True)

    e1c, e2c, k2c = column(e1), column(e2), column(k2)
    same_group = (row_i // seq) == (col_i // seq)
    earlier = same_group & (row_i < col_i)
    one = jnp.int32(1)
    pos1 = jnp.sum(jnp.where(earlier & (e1c == e1), one, 0), axis=0, keepdims=True)
    count1 = jnp.sum(jnp.where(same_group & (e1c == e2), one, 0), axis=0, keepdims=True)
    before2 = jnp.sum(jnp.where(earlier & (e2c == e2) & (k2c > 0), one, 0), axis=0, keepdims=True)
    pos2 = count1 + before2
    lane = iota((1, tokens), 1)
    group_base = (lane // seq) * cap
    kept1 = pos1 < cap
    kept2 = (pos2 < cap) & (k2 > 0)
    place1 = jnp.where(kept1, group_base + pos1, -1)
    place2 = jnp.where(kept2, group_base + pos2, -1)

    def slot_of(expert):
        apart = expert ^ me
        top = apart // plane
        quarter = jnp.where(top == order[0], 0, jnp.where(top == order[3], 3, top + 1))
        return quarter * plane + apart % plane

    key1 = jnp.where(kept1, slot_of(e1) * rows + place1, -1)
    key2 = jnp.where(kept2, slot_of(e2) * rows + place2, -1)
    slot_i = iota((slots, tokens), 0)
    disp = ((slot_i == key1) | (slot_i == key2)).astype(F32).astype(BF16)

    fetched[3].wait()
    x = x_ref[...]
    first_rows = plane * rows
    sx[0:first_rows, :] = dot(disp[0:first_rows], x).astype(BF16)

    pl.semaphore_wait(barrier, n - 1)

    def one_row(src, dst, src_row, send, recv, q, d):
        return pltpu.make_async_remote_copy(src.at[pl.ds(src_row, 1)], dst.at[pl.ds(me, 1)], send.at[q], recv.at[0], device_id=(d,), device_id_type=MESH)

    def block(src, dst, send, recv, half_i, q, d):
        at = pl.ds(q * rows, rows)
        return pltpu.make_async_remote_copy(src.at[at], dst.at[at], send.at[half_i], recv.at[half_i], device_id=(d,), device_id_type=MESH)

    def own_row(src, dst, src_row, recv):
        pltpu.make_async_copy(src.at[pl.ds(src_row, 1)], dst.at[pl.ds(me, 1)], recv.at[0]).start()

    def own_block(src, dst, recv):
        pltpu.make_async_copy(src.at[pl.ds(own, rows)], dst.at[pl.ds(own, rows)], recv.at[near]).start()

    def settle(ref, sem, rows_at):
        pltpu.make_async_copy(ref.at[rows_at], ref.at[rows_at], sem).wait()

    def group_at(c):
        return pl.ds(*span[c])

    def send_group(src, dst, send, recv, c, pieces=None):
        each_partner(pieces or quarters_of[c], lambda q, d: block(src, dst, send, recv, c, q, d).start())

    send_group(sx, xe, s_x, v_x, early)
    sx[first_rows:, :] = dot(disp[first_rows:], x).astype(BF16)
    send_group(sx, xe, s_x, v_x, near)
    own_block(sx, xe, v_x)
    fetched[4].wait()
    fetched[5].wait()

    expert_i = iota((n, tokens), 0)
    hot1 = (expert_i == e1).astype(F32)
    hot2 = (expert_i == e2).astype(F32)
    place_i = iota((128, tokens), 0)
    at1 = (place_i == place1).astype(F32)
    at2 = (place_i == place2).astype(F32)

    wgt = wg_ref[...]
    logits = dot(wgt, x, NT)
    top_logit = jnp.max(logits, axis=0, keepdims=True)
    expd = jnp.exp(logits - top_logit)
    prob = expd / jnp.sum(expd, axis=0, keepdims=True)
    g1 = jnp.sum(prob * hot1, axis=0, keepdims=True)
    g2 = jnp.sum(prob * hot2, axis=0, keepdims=True)
    gsum = g1 + g2
    ratio1, ratio2 = g1 / gsum, g2 / gsum
    n1 = ratio1.astype(BF16).astype(F32)
    n2 = ratio2.astype(BF16).astype(F32)
    mix = ratio1 * ratio2
    exact = lax.Precision.HIGHEST
    expert_f = expert_i.astype(F32)
    e1f, e2f = jnp.sum(hot1 * expert_f, axis=0, keepdims=True), jnp.sum(hot2 * expert_f, axis=0, keepdims=True)

    def placed(place, base):
        return (place_i == jnp.where(place >= 0, place + base, -1)).astype(F32)

    norm_rows = dot(hot1 * n1, at1, NT, precision=exact) + dot(hot2 * n2, at2, NT, precision=exact)
    norm_rows = norm_rows + dot(hot1 * mix, placed(place1, 16), NT, precision=exact) + dot(hot2 * mix, placed(place2, 16), NT, precision=exact)
    norm_rows = norm_rows + dot(hot1 * e2f, placed(place1, 104), NT, precision=exact) + dot(hot2 * e1f, placed(place2, 104), NT, precision=exact)
    sub_n, lane_n = iota((n, 128), 0), iota((n, 128), 1)

    def as_lanes(col, base):
        return jnp.sum(jnp.where(lane_n == sub_n + base, col, 0.0), axis=0, keepdims=True)

    def as_column(row, base):
        return jnp.sum(jnp.where(lane_n == sub_n + base, row, 0.0), axis=1, keepdims=True)

    r = r_ref[...]
    xr = jnp.sum(jnp.sum(x.astype(F32) * r.astype(F32), axis=0, keepdims=True), axis=1, keepdims=True)
    lane_1 = iota((1, 128), 1)
    stats = as_lanes(jnp.sum(hot1, axis=1, keepdims=True), 32) + as_lanes(jnp.sum(prob, axis=1, keepdims=True), 64) + jnp.where(lane_1 == 96, xr, 0.0)
    rows_s[...] = norm_rows + stats

    sr[...] = dot(disp, r).astype(BF16)
    each_partner(everyone, lambda q, d: one_row(rows_s, rows_r, d, s_row, v_row, q, d).start())
    own_row(rows_s, rows_r, me, v_row)
    send_group(sr, re, s_r, v_r, early)
    send_group(sx, xe, s_x, v_x, late)
    send_group(sr, re, s_r, v_r, near)
    own_block(sr, re, v_r)
    send_group(sr, re, s_r, v_r, late)

    slot_row = iota((slots, n), 0)
    quarter = slot_row // rows // plane
    far = jnp.where(quarter == 0, order[0], jnp.where(quarter == 3, order[3], quarter - 1))
    source = (far * plane + slot_row // rows % plane) ^ me
    pick = (source == iota((slots, n), 1)).astype(F32)
    lane_s, row_s = iota((slots, 128), 1), iota((slots, 128), 0) % rows
    mine = lane_s == row_s
    key1c, key2c = column(key1), column(key2)
    slot_l = iota((tokens, slots), 1)
    comb = ((slot_l == key1c) | (slot_l == key2c)).astype(F32).astype(BF16)
    fetched[6].wait()
    fetched[7].wait()

    def forward(c):
        at = group_at(c)
        settle(xe, v_x.at[c], at)
        pre = dot(xe[at, :], w1[...])
        sq = pre * pre
        th = jnp.tanh(GELU_C * (pre + GELU_K * (sq * pre)))
        cdf = 0.5 * (1.0 + th)
        slope[at, :] = cdf + (0.5 * GELU_C) * pre * (1.0 - th * th) * (1.0 + 3 * GELU_K * sq)
        act[at, :] = (pre * cdf).astype(BF16)
        hid[at, :] = dot(act[at, :], w2[...]).astype(BF16)

    def receive(c):
        at = group_at(c)
        start, size = span[c]
        settle(re, v_r.at[c], at)
        rc = re[at, :].astype(F32)
        norm = norms[start:start + size]
        gy[at, :] = (norm * rc).astype(BF16)
        d = jnp.sum(hid[at, :].astype(F32) * rc, axis=1, keepdims=True)
        share = mixes[start:start + size] * d.astype(BF16).astype(F32) * signs[start:start + size]
        part_s[...] += dot(share.astype(BF16), xe[at, :], TN)
        in_lane = jnp.where(mine[start:start + size], d, 0.0)
        dots_s[pl.ds(start // rows, size // rows), :] = jnp.sum(in_lane.reshape(size // rows, rows, 128), axis=1)
        return jnp.sum(norm * d, axis=0, keepdims=True)

    def backward(c):
        at = group_at(c)
        ga = dot(gy[at, :], w2[...], NT).astype(BF16)
        gpre[at, :] = (ga.astype(F32) * slope[at, :]).astype(BF16)
        gs[at, :] = dot(gpre[at, :], w1[...], NT).astype(BF16)

    def send_back(c, pieces=None):
        send_group(gs, gback, s_g, v_g, c, pieces)

    forward(early)
    forward(near)
    settle(rows_r, v_row.at[0], pl.ds(0, n))
    all_rows = rows_r[...]
    total = jnp.sum(all_rows, axis=0, keepdims=True)
    frac = as_column(total, 32) / tokens_all
    mean_prob = as_column(total, 64) / tokens_all
    wide = dot(pick, all_rows, precision=exact)
    norms = jnp.sum(jnp.where(mine, wide, 0.0), axis=1, keepdims=True)
    mixes = jnp.sum(jnp.where(lane_s == row_s + 16, wide, 0.0), axis=1, keepdims=True)
    others = jnp.sum(jnp.where(lane_s == row_s + 104, wide, 0.0), axis=1, keepdims=True)
    column_i = iota((slots, n), 1)
    signs = (column_i == me).astype(F32) - (column_i.astype(F32) == others).astype(F32)
    aux_prob = (ALPHA * hidden * n) * frac
    aux_log = prob * (aux_prob - jnp.sum(prob * aux_prob, axis=0, keepdims=True))
    part_s[...] = dot(aux_log.astype(BF16), x_ref[...])

    loss_part = receive(early)
    backward(early)
    split_early, split_late = 5, 2
    send_back(early, ((0, 0, split_early),))
    loss_part = loss_part + receive(near)
    backward(near)
    send_back(near)
    own_block(gs, gback, v_g)
    forward(late)
    xet[...] = jnp.transpose(xe[...])
    loss_part = loss_part + receive(late)
    dots_s[...] = dots_s[...] + jnp.where(lane_1 == 16, loss_part, 0.0)

    share_rows = n // plane

    def line_copy(src, src_row, dst, dst_row, send, recv, q, d):
        return pltpu.make_async_remote_copy(src.at[pl.ds(src_row, 1)], dst.at[pl.ds(dst_row, 1)], send.at[q], recv.at[0], device_id=(d,), device_id_type=MESH)

    def own_line(src, src_row, dst, dst_row, recv):
        pltpu.make_async_copy(src.at[pl.ds(src_row, 1)], dst.at[pl.ds(dst_row, 1)], recv.at[0]).start()

    def plane_peers(body):
        @pl.loop(1, plane)
        def _(step):
            d = partner(1, step)
            for j in range(share_rows):
                body(step * share_rows + j, d, lax.rem(d, plane) * share_rows + j, low * share_rows + j, j)

    def scatter(q, d, theirs, ours, j):
        return line_copy(part_s, theirs, part_r, ours, s_part, v_part, q, d)

    def line_peers(body):
        for quarter in (0, 3, 2):
            d = partner(quarter, 0)
            for j in range(share_rows):
                body(quarter * share_rows + j, d, j)

    def exchange(q, d, j):
        return line_copy(mid_s, j, mid_r, high * share_rows + j, s_mid, v_mid, q, d)

    def gather(q, d, theirs, ours, j):
        return line_copy(sum_s, j, gg_ref, ours, s_sum, v_sum, q, d)

    plane_peers(lambda *a: scatter(*a).start())
    for j in range(share_rows):
        own_line(part_s, low * share_rows + j, part_r, low * share_rows + j, v_part)
    each_partner(everyone, lambda q, d: one_row(dots_s, dots_r, q, s_dot, v_dot, q, d).start())
    own_row(dots_s, dots_r, plane, v_dot)
    send_back(early, ((0, split_early, plane),))
    backward(late)
    send_back(late, ((3, 0, split_late),))
    gw1[...] = dot(xet[...], gpre[...]).astype(BF16)

    settle(part_r, v_part.at[0], pl.ds(0, n))
    fold = part_r[0:8, :] + part_r[8:16, :] + part_r[16:24, :] + part_r[24:32, :]
    mid_s[0:4, :] = fold[0:4] + fold[4:8]
    line_peers(lambda *a: exchange(*a).start())
    for j in range(share_rows):
        own_line(mid_s, j, mid_r, high * share_rows + j, v_mid)
    send_back(late, ((3, split_late, plane),))
    gw2[...] = dot(act[...], gy[...], TN).astype(BF16)

    settle(mid_r, v_mid.at[0], pl.ds(0, 16))
    fold = mid_r[0:8, :] + mid_r[8:16, :]
    sum_s[0:4, :] = fold[0:4] + fold[4:8]
    plane_peers(lambda *a: gather(*a).start())
    for j in range(share_rows):
        own_line(sum_s, j, gg_ref, low * share_rows + j, v_sum)

    settle(dots_r, v_dot.at[0], pl.ds(0, n))
    all_dots = dots_r[...]
    d1 = jnp.sum(dot(all_dots, hot1, TN, precision=exact) * at1, axis=0, keepdims=True)
    d2 = jnp.sum(dot(all_dots, hot2, TN, precision=exact) * at2, axis=0, keepdims=True)
    apart = d1.astype(BF16).astype(F32) - d2.astype(BF16).astype(F32)
    glog = (aux_log + (mix * apart) * (hot1 - hot2)).astype(BF16)

    both = jnp.sum(jnp.where(lane_1 == 96, total, 0.0), axis=1, keepdims=True)
    both = both + jnp.sum(jnp.where(lane_1 == 16, jnp.sum(all_dots, axis=0, keepdims=True), 0.0), axis=1, keepdims=True)
    aux = jnp.sum(frac * mean_prob, axis=0, keepdims=True) * n
    loss_ref[...] = jnp.broadcast_to(both / numel + ALPHA * aux, loss_ref.shape)
    out = r_ref[...].astype(F32) + dot(glog, wg_ref[...], TN)
    for c in (near, early, late):
        start, size = span[c]
        settle(gback, v_g.at[c], group_at(c))
        out = out + dot(comb[:, start:start + size], gback[group_at(c), :])
    gx_ref[...] = out.astype(BF16)

    settle(gg_ref, v_sum.at[0], pl.ds(0, n))
    each_partner(everyone, lambda q, d: one_row(rows_s, rows_r, d, s_row, v_row, q, d).wait_send())
    each_partner(everyone, lambda q, d: one_row(dots_s, dots_r, q, s_dot, v_dot, q, d).wait_send())
    plane_peers(lambda *a: scatter(*a).wait_send())
    line_peers(lambda *a: exchange(*a).wait_send())
    plane_peers(lambda *a: gather(*a).wait_send())
    for ref, sem in ((sx, s_x), (sr, s_r), (gs, s_g)):
        settle(ref, sem.at[early], group_at(early))
        settle(ref, sem.at[near], pl.ds(own + rows, span[near][1] - rows))
        settle(ref, sem.at[late], group_at(late))


def solution(mesh):
    n = mesh.shape['ep']

    def layer_body(x_loc, r_loc, w_gate, w_in_loc, w_out_loc, first_ids, second_ids, keep_ids):
        groups, seq, hidden = x_loc.shape
        cap = 2 * seq // w_gate.shape[1]
        ff = w_in_loc.shape[2]
        tokens = groups * seq
        slots = n * groups * cap
        vmem = pl.BlockSpec(memory_space=pltpu.VMEM)
        hbm = pl.BlockSpec(memory_space=pltpu.HBM)
        dma = pltpu.SemaphoreType.DMA
        out = pl.pallas_call(
            functools.partial(layer_kernel, n, cap, seq),
            name='moe_layer',
            out_shape=(
                pltpu.VMEM((8, 128), F32),
                pltpu.VMEM((tokens, hidden), BF16),
                pltpu.VMEM((n, hidden), F32),
                pltpu.VMEM((hidden, ff), BF16),
                pltpu.VMEM((ff, hidden), BF16),
            ),
            in_specs=[hbm] * 8,
            out_specs=(vmem,) * 5,
            scratch_shapes=[
                pltpu.VMEM((groups, seq), jnp.int32),
                pltpu.VMEM((groups, seq), jnp.int32),
                pltpu.VMEM((groups, seq), jnp.int32),
                pltpu.VMEM((tokens, hidden), BF16),
                pltpu.VMEM((tokens, hidden), BF16),
                pltpu.VMEM((n, hidden), BF16),
                pltpu.VMEM((hidden, ff), BF16),
                pltpu.VMEM((ff, hidden), BF16),
                pltpu.VMEM((slots, hidden), BF16),
                pltpu.VMEM((slots, hidden), BF16),
                pltpu.VMEM((slots, hidden), BF16),
                pltpu.VMEM((slots, hidden), BF16),
                pltpu.VMEM((slots, hidden), BF16),
                pltpu.VMEM((slots, ff), BF16),
                pltpu.VMEM((slots, ff), BF16),
                pltpu.VMEM((slots, hidden), BF16),
                pltpu.VMEM((slots, hidden), BF16),
                pltpu.VMEM((n, 128), F32),
                pltpu.VMEM((n, 128), F32),
                pltpu.VMEM((n, 128), F32),
                pltpu.VMEM((n, 128), F32),
                pltpu.VMEM((n, hidden), F32),
                pltpu.VMEM((n, hidden), F32),
                pltpu.VMEM((8, hidden), F32),
                pltpu.VMEM((16, hidden), F32),
                pltpu.VMEM((8, hidden), F32),
                pltpu.VMEM((slots, ff), F32),
                pltpu.VMEM((slots, hidden), BF16),
                pltpu.VMEM((hidden, slots), BF16),
                dma((8,)),
                dma((3,)), dma((3,)), dma((3,)), dma((n,)), dma((n,)), dma((n,)), dma((16,)), dma((n,)),
                dma((3,)), dma((3,)), dma((3,)), dma((1,)), dma((1,)), dma((1,)), dma((1,)), dma((1,)),
            ],
            compiler_params=pltpu.CompilerParams(collective_id=0, has_side_effects=True, vmem_limit_bytes=44 * 1024 * 1024),
        )(*(pltpu.with_memory_space_constraint(a, pltpu.HBM) for a in (
            first_ids, second_ids, keep_ids, x_loc.reshape(tokens, hidden), r_loc.reshape(tokens, hidden), w_gate.T, w_in_loc[0], w_out_loc[0])))
        loss, gx, gg, gw1, gw2 = pl.pallas_call(
            write_kernel,
            name='write_results',
            out_shape=(
                jax.ShapeDtypeStruct((1, 1), F32),
                jax.ShapeDtypeStruct((tokens, hidden), BF16),
                jax.ShapeDtypeStruct((n, hidden), F32),
                jax.ShapeDtypeStruct((hidden, ff), BF16),
                jax.ShapeDtypeStruct((ff, hidden), BF16),
            ),
            in_specs=[vmem] * 5,
            out_specs=(pl.BlockSpec(memory_space=pltpu.SMEM), hbm, hbm, hbm, hbm),
            scratch_shapes=[dma((4,))],
            compiler_params=pltpu.CompilerParams(vmem_limit_bytes=2 * 1024 * 1024),
        )(*(pltpu.with_memory_space_constraint(a, pltpu.VMEM) for a in out))
        return loss.reshape(()), gx.reshape(x_loc.shape), gw1[None], gw2[None], gg.T

    row_spec = P('ep', None, None)
    id_spec = P('ep', None)
    return jax.shard_map(layer_body, mesh=mesh, in_specs=(row_spec, row_spec, P(None, None), row_spec, row_spec, id_spec, id_spec, id_spec), out_specs=(P(), row_spec, row_spec, row_spec, P(None, None)), check_vma=False)
```

```python
import functools

import jax
import jax.numpy as jnp
from jax import lax
from jax.experimental import pallas as pl
from jax.experimental.pallas import tpu as pltpu
from jax.sharding import PartitionSpec as P

ALPHA = 0.01
MESH = pl.DeviceIdType.MESH
F32 = jnp.float32
BF16 = jnp.bfloat16
NN = (((1,), (0,)), ((), ()))
NT = (((1,), (1,)), ((), ()))
TN = (((0,), (0,)), ((), ()))
GELU_C = 0.7978845608028654
GELU_K = 0.044715


def dot(a, b, dims=NN, **kw):
    return lax.dot_general(a, b, dims, preferred_element_type=F32, **kw)


def iota(shape, dim):
    return lax.broadcasted_iota(jnp.int32, shape, dim)


def flip_bits(a, b):
    return a + b - 2 * a * b


def write_kernel(loss_v, gx_v, gg_v, gw1_v, gw2_v, loss_s, gx_h, gg_h, gw1_h, gw2_h, sem):
    copies = [pltpu.make_async_copy(src, dst, sem.at[i]) for i, (src, dst) in enumerate(((gw1_v, gw1_h), (gw2_v, gw2_h), (gx_v, gx_h), (gg_v, gg_h)))]
    for copy in copies:
        copy.start()
    loss_s[0, 0] = jnp.max(loss_v[...])
    for copy in copies:
        copy.wait()


def layer_kernel(n, cap, seq, e1_hbm, e2_hbm, k2_hbm, x_hbm, r_hbm, wg_hbm, w1_hbm, w2_hbm,
                 loss_ref, gx_ref, gg_ref, gw1, gw2,
                 e1_ref, e2_ref, k2_ref, x_ref, r_ref, wg_ref, w1, w2, sx, sr, xe, re, gy, act, gpre, gs, gback,
                 rows_s, rows_r, dots_s, dots_r, part_s, part_r, mid_s, mid_r, sum_s, slope, hid, xet, in_sem,
                 s_x, s_r, s_g, s_row, s_dot, s_part, s_mid, s_sum,
                 v_x, v_r, v_g, v_row, v_dot, v_part, v_mid, v_sum):
    me = lax.axis_index('ep')
    tokens, hidden = x_ref.shape
    ff = w1.shape[1]
    groups = tokens // seq
    rows = groups * cap
    slots = n * rows
    plane = n // 4
    tokens_all = tokens * n
    numel = tokens_all * hidden

    low, high = lax.rem(me, plane), lax.div(me, plane)
    low_bits = [lax.rem(low, 2), lax.rem(lax.div(low, 2), 2), lax.div(low, 4)]
    high_bits = [lax.rem(high, 2), lax.div(high, 2)]
    order = (2, 0, 1, 3)
    own = plane * rows

    def partner(quarter, step):
        far = order[quarter]
        top = [bit if not (far >> i) & 1 else 1 - bit for i, bit in enumerate(high_bits)]
        step_bits = [lax.rem(step, 2), lax.rem(lax.div(step, 2), 2), lax.div(step, 4)]
        bits = [flip_bits(a, b) for a, b in zip(low_bits, step_bits)]
        return (top[0] + 2 * top[1]) * plane + bits[0] + 2 * bits[1] + 4 * bits[2]

    def each_partner(pieces, body):
        for quarter, lo, hi in pieces:
            first = max(lo, 1) if order[quarter] == 0 else lo

            @pl.loop(first, hi)
            def _(step):
                body(quarter * plane + step, partner(quarter, step))

    everyone = tuple((quarter, 0, plane) for quarter in (0, 3, 1, 2))
    early, near, late = 0, 1, 2
    quarters_of = (((0, 0, plane),), ((1, 0, plane), (2, 0, plane)), ((3, 0, plane),))
    span = ((0, plane * rows), (plane * rows, 2 * plane * rows), (3 * plane * rows, plane * rows))

    barrier = pltpu.get_barrier_semaphore()
    each_partner(everyone, lambda q, d: pl.semaphore_signal(barrier, inc=1, device_id=(d,), device_id_type=MESH))
    fetched = [pltpu.make_async_copy(src, dst, in_sem.at[i]) for i, (src, dst) in enumerate((
        (e1_hbm, e1_ref), (e2_hbm, e2_ref), (k2_hbm, k2_ref), (x_hbm, x_ref), (r_hbm, r_ref), (wg_hbm, wg_ref), (w1_hbm, w1), (w2_hbm, w2)))]
    for copy in fetched:
        copy.start()
    for copy in fetched[:3]:
        copy.wait()

    spread = (iota((seq, tokens), 1) % seq == iota((seq, tokens), 0)).astype(F32).astype(BF16)
    own_group = iota((groups, tokens), 1) // seq == iota((groups, tokens), 0)

    def along_lanes(ref):
        wide = dot(ref[...].astype(F32).astype(BF16), spread)
        return jnp.sum(jnp.where(own_group, wide, 0.0), axis=0, keepdims=True).astype(jnp.int32)

    e1, e2, k2 = along_lanes(e1_ref), along_lanes(e2_ref), along_lanes(k2_ref)
    row_i, col_i = iota((tokens, tokens), 0), iota((tokens, tokens), 1)
    eye = row_i == col_i

    def column(row):
        return jnp.sum(jnp.where(eye, row, 0), axis=1, keepdims=True)

    e1c, e2c, k2c = column(e1), column(e2), column(k2)
    same_group = (row_i // seq) == (col_i // seq)
    earlier = same_group & (row_i < col_i)
    one = jnp.int32(1)
    pos1 = jnp.sum(jnp.where(earlier & (e1c == e1), one, 0), axis=0, keepdims=True)
    count1 = jnp.sum(jnp.where(same_group & (e1c == e2), one, 0), axis=0, keepdims=True)
    before2 = jnp.sum(jnp.where(earlier & (e2c == e2) & (k2c > 0), one, 0), axis=0, keepdims=True)
    pos2 = count1 + before2
    lane = iota((1, tokens), 1)
    group_base = (lane // seq) * cap
    kept1 = pos1 < cap
    kept2 = (pos2 < cap) & (k2 > 0)
    place1 = jnp.where(kept1, group_base + pos1, -1)
    place2 = jnp.where(kept2, group_base + pos2, -1)

    def slot_of(expert):
        apart = expert ^ me
        top = apart // plane
        quarter = jnp.where(top == order[0], 0, jnp.where(top == order[3], 3, top + 1))
        return quarter * plane + apart % plane

    key1 = jnp.where(kept1, slot_of(e1) * rows + place1, -1)
    key2 = jnp.where(kept2, slot_of(e2) * rows + place2, -1)
    slot_i = iota((slots, tokens), 0)
    disp = ((slot_i == key1) | (slot_i == key2)).astype(F32).astype(BF16)

    fetched[3].wait()
    x = x_ref[...]
    first_rows = plane * rows
    sx[0:first_rows, :] = dot(disp[0:first_rows], x).astype(BF16)

    pl.semaphore_wait(barrier, n - 1)

    def one_row(src, dst, src_row, send, recv, q, d):
        return pltpu.make_async_remote_copy(src.at[pl.ds(src_row, 1)], dst.at[pl.ds(me, 1)], send.at[q], recv.at[0], device_id=(d,), device_id_type=MESH)

    def block(src, dst, send, recv, half_i, q, d):
        at = pl.ds(q * rows, rows)
        return pltpu.make_async_remote_copy(src.at[at], dst.at[at], send.at[half_i], recv.at[half_i], device_id=(d,), device_id_type=MESH)

    def own_row(src, dst, src_row, recv):
        pltpu.make_async_copy(src.at[pl.ds(src_row, 1)], dst.at[pl.ds(me, 1)], recv.at[0]).start()

    def own_block(src, dst, recv):
        pltpu.make_async_copy(src.at[pl.ds(own, rows)], dst.at[pl.ds(own, rows)], recv.at[near]).start()

    def settle(ref, sem, rows_at):
        pltpu.make_async_copy(ref.at[rows_at], ref.at[rows_at], sem).wait()

    def group_at(c):
        return pl.ds(*span[c])

    def send_group(src, dst, send, recv, c, pieces=None):
        each_partner(pieces or quarters_of[c], lambda q, d: block(src, dst, send, recv, c, q, d).start())

    send_group(sx, xe, s_x, v_x, early)
    sx[first_rows:, :] = dot(disp[first_rows:], x).astype(BF16)
    send_group(sx, xe, s_x, v_x, near)
    own_block(sx, xe, v_x)
    fetched[4].wait()
    fetched[5].wait()

    expert_i = iota((n, tokens), 0)
    hot1 = (expert_i == e1).astype(F32)
    hot2 = (expert_i == e2).astype(F32)
    place_i = iota((128, tokens), 0)
    at1 = (place_i == place1).astype(F32)
    at2 = (place_i == place2).astype(F32)

    wgt = wg_ref[...]
    logits = dot(wgt, x, NT)
    top_logit = jnp.max(logits, axis=0, keepdims=True)
    expd = jnp.exp(logits - top_logit)
    prob = expd / jnp.sum(expd, axis=0, keepdims=True)
    g1 = jnp.sum(prob * hot1, axis=0, keepdims=True)
    g2 = jnp.sum(prob * hot2, axis=0, keepdims=True)
    gsum = g1 + g2
    ratio1, ratio2 = g1 / gsum, g2 / gsum
    n1 = ratio1.astype(BF16).astype(F32)
    n2 = ratio2.astype(BF16).astype(F32)
    mix = ratio1 * ratio2
    exact = lax.Precision.HIGHEST
    expert_f = expert_i.astype(F32)
    e1f, e2f = jnp.sum(hot1 * expert_f, axis=0, keepdims=True), jnp.sum(hot2 * expert_f, axis=0, keepdims=True)

    def placed(place, base):
        return (place_i == jnp.where(place >= 0, place + base, -1)).astype(F32)

    norm_rows = dot(hot1 * n1, at1, NT, precision=exact) + dot(hot2 * n2, at2, NT, precision=exact)
    norm_rows = norm_rows + dot(hot1 * mix, placed(place1, 16), NT, precision=exact) + dot(hot2 * mix, placed(place2, 16), NT, precision=exact)
    norm_rows = norm_rows + dot(hot1 * e2f, placed(place1, 104), NT, precision=exact) + dot(hot2 * e1f, placed(place2, 104), NT, precision=exact)
    sub_n, lane_n = iota((n, 128), 0), iota((n, 128), 1)

    def as_lanes(col, base):
        return jnp.sum(jnp.where(lane_n == sub_n + base, col, 0.0), axis=0, keepdims=True)

    def as_column(row, base):
        return jnp.sum(jnp.where(lane_n == sub_n + base, row, 0.0), axis=1, keepdims=True)

    r = r_ref[...]
    xr = jnp.sum(jnp.sum(x.astype(F32) * r.astype(F32), axis=0, keepdims=True), axis=1, keepdims=True)
    lane_1 = iota((1, 128), 1)
    stats = as_lanes(jnp.sum(hot1, axis=1, keepdims=True), 32) + as_lanes(jnp.sum(prob, axis=1, keepdims=True), 64) + jnp.where(lane_1 == 96, xr, 0.0)
    rows_s[...] = norm_rows + stats

    sr[...] = dot(disp, r).astype(BF16)
    each_partner(everyone, lambda q, d: one_row(rows_s, rows_r, d, s_row, v_row, q, d).start())
    own_row(rows_s, rows_r, me, v_row)
    send_group(sr, re, s_r, v_r, early)
    send_group(sx, xe, s_x, v_x, late)
    send_group(sr, re, s_r, v_r, near)
    own_block(sr, re, v_r)
    send_group(sr, re, s_r, v_r, late)

    slot_row = iota((slots, n), 0)
    quarter = slot_row // rows // plane
    far = jnp.where(quarter == 0, order[0], jnp.where(quarter == 3, order[3], quarter - 1))
    source = (far * plane + slot_row // rows % plane) ^ me
    pick = (source == iota((slots, n), 1)).astype(F32)
    lane_s, row_s = iota((slots, 128), 1), iota((slots, 128), 0) % rows
    mine = lane_s == row_s
    key1c, key2c = column(key1), column(key2)
    slot_l = iota((tokens, slots), 1)
    comb = ((slot_l == key1c) | (slot_l == key2c)).astype(F32).astype(BF16)
    fetched[6].wait()
    fetched[7].wait()

    def forward(c):
        at = group_at(c)
        settle(xe, v_x.at[c], at)
        pre = dot(xe[at, :], w1[...])
        sq = pre * pre
        th = jnp.tanh(GELU_C * (pre + GELU_K * (sq * pre)))
        cdf = 0.5 * (1.0 + th)
        slope[at, :] = cdf + (0.5 * GELU_C) * pre * (1.0 - th * th) * (1.0 + 3 * GELU_K * sq)
        act[at, :] = (pre * cdf).astype(BF16)
        hid[at, :] = dot(act[at, :], w2[...]).astype(BF16)

    def receive(c):
        at = group_at(c)
        start, size = span[c]
        settle(re, v_r.at[c], at)
        rc = re[at, :].astype(F32)
        norm = norms[start:start + size]
        gy[at, :] = (norm * rc).astype(BF16)
        d = jnp.sum(hid[at, :].astype(F32) * rc, axis=1, keepdims=True)
        share = mixes[start:start + size] * d.astype(BF16).astype(F32) * signs[start:start + size]
        part_s[...] += dot(share.astype(BF16), xe[at, :], TN)
        in_lane = jnp.where(mine[start:start + size], d, 0.0)
        dots_s[pl.ds(start // rows, size // rows), :] = jnp.sum(in_lane.reshape(size // rows, rows, 128), axis=1)
        return jnp.sum(norm * d, axis=0, keepdims=True)

    def backward(c):
        at = group_at(c)
        ga = dot(gy[at, :], w2[...], NT).astype(BF16)
        gpre[at, :] = (ga.astype(F32) * slope[at, :]).astype(BF16)
        gs[at, :] = dot(gpre[at, :], w1[...], NT).astype(BF16)

    def send_back(c, pieces=None):
        send_group(gs, gback, s_g, v_g, c, pieces)

    forward(early)
    forward(near)
    settle(rows_r, v_row.at[0], pl.ds(0, n))
    all_rows = rows_r[...]
    total = jnp.sum(all_rows, axis=0, keepdims=True)
    frac = as_column(total, 32) / tokens_all
    mean_prob = as_column(total, 64) / tokens_all
    wide = dot(pick, all_rows, precision=exact)
    norms = jnp.sum(jnp.where(mine, wide, 0.0), axis=1, keepdims=True)
    mixes = jnp.sum(jnp.where(lane_s == row_s + 16, wide, 0.0), axis=1, keepdims=True)
    others = jnp.sum(jnp.where(lane_s == row_s + 104, wide, 0.0), axis=1, keepdims=True)
    column_i = iota((slots, n), 1)
    signs = (column_i == me).astype(F32) - (column_i.astype(F32) == others).astype(F32)
    aux_prob = (ALPHA * hidden * n) * frac
    aux_log = prob * (aux_prob - jnp.sum(prob * aux_prob, axis=0, keepdims=True))
    part_s[...] = dot(aux_log.astype(BF16), x_ref[...])

    loss_part = receive(early)
    backward(early)
    split_late = 1
    send_back(early)
    loss_part = loss_part + receive(near)
    backward(near)
    send_back(near)
    own_block(gs, gback, v_g)
    forward(late)
    xet[...] = jnp.transpose(xe[...])
    loss_part = loss_part + receive(late)
    dots_s[...] = dots_s[...] + jnp.where(lane_1 == 16, loss_part, 0.0)

    share_rows = n // plane

    def line_copy(src, src_row, dst, dst_row, send, recv, q, d):
        return pltpu.make_async_remote_copy(src.at[pl.ds(src_row, 1)], dst.at[pl.ds(dst_row, 1)], send.at[q], recv.at[0], device_id=(d,), device_id_type=MESH)

    def own_line(src, src_row, dst, dst_row, recv):
        pltpu.make_async_copy(src.at[pl.ds(src_row, 1)], dst.at[pl.ds(dst_row, 1)], recv.at[0]).start()

    def plane_peers(body):
        @pl.loop(1, plane)
        def _(step):
            d = partner(1, step)
            for j in range(share_rows):
                body(step * share_rows + j, d, lax.rem(d, plane) * share_rows + j, low * share_rows + j, j)

    def scatter(q, d, theirs, ours, j):
        return line_copy(part_s, theirs, part_r, ours, s_part, v_part, q, d)

    def line_peers(body):
        for quarter in (0, 3, 2):
            d = partner(quarter, 0)
            for j in range(share_rows):
                body(quarter * share_rows + j, d, j)

    def exchange(q, d, j):
        return line_copy(mid_s, j, mid_r, high * share_rows + j, s_mid, v_mid, q, d)

    def gather(q, d, theirs, ours, j):
        return line_copy(sum_s, j, gg_ref, ours, s_sum, v_sum, q, d)

    plane_peers(lambda *a: scatter(*a).start())
    for j in range(share_rows):
        own_line(part_s, low * share_rows + j, part_r, low * share_rows + j, v_part)
    each_partner(everyone, lambda q, d: one_row(dots_s, dots_r, q, s_dot, v_dot, q, d).start())
    own_row(dots_s, dots_r, plane, v_dot)
    backward(late)
    send_back(late, ((3, 0, split_late),))
    settle(part_r, v_part.at[0], pl.ds(0, n))
    fold = part_r[0:8, :] + part_r[8:16, :] + part_r[16:24, :] + part_r[24:32, :]
    mid_s[0:4, :] = fold[0:4] + fold[4:8]
    line_peers(lambda *a: exchange(*a).start())
    for j in range(share_rows):
        own_line(mid_s, j, mid_r, high * share_rows + j, v_mid)
    send_back(late, ((3, split_late, plane),))
    gw1[...] = dot(xet[...], gpre[...]).astype(BF16)
    gw2[...] = dot(act[...], gy[...], TN).astype(BF16)

    settle(mid_r, v_mid.at[0], pl.ds(0, 16))
    fold = mid_r[0:8, :] + mid_r[8:16, :]
    sum_s[0:4, :] = fold[0:4] + fold[4:8]
    plane_peers(lambda *a: gather(*a).start())
    for j in range(share_rows):
        own_line(sum_s, j, gg_ref, low * share_rows + j, v_sum)

    settle(dots_r, v_dot.at[0], pl.ds(0, n))
    all_dots = dots_r[...]
    d1 = jnp.sum(dot(all_dots, hot1, TN, precision=exact) * at1, axis=0, keepdims=True)
    d2 = jnp.sum(dot(all_dots, hot2, TN, precision=exact) * at2, axis=0, keepdims=True)
    apart = d1.astype(BF16).astype(F32) - d2.astype(BF16).astype(F32)
    glog = (aux_log + (mix * apart) * (hot1 - hot2)).astype(BF16)

    both = jnp.sum(jnp.where(lane_1 == 96, total, 0.0), axis=1, keepdims=True)
    both = both + jnp.sum(jnp.where(lane_1 == 16, jnp.sum(all_dots, axis=0, keepdims=True), 0.0), axis=1, keepdims=True)
    aux = jnp.sum(frac * mean_prob, axis=0, keepdims=True) * n
    loss_ref[...] = jnp.broadcast_to(both / numel + ALPHA * aux, loss_ref.shape)
    out = r_ref[...].astype(F32) + dot(glog, wg_ref[...], TN)
    each_partner(everyone, lambda q, d: one_row(rows_s, rows_r, d, s_row, v_row, q, d).wait_send())
    each_partner(everyone, lambda q, d: one_row(dots_s, dots_r, q, s_dot, v_dot, q, d).wait_send())
    plane_peers(lambda *a: scatter(*a).wait_send())
    line_peers(lambda *a: exchange(*a).wait_send())

    def sent(ref, sem, groups_sent):
        for c in groups_sent:
            start, size = span[c]
            settle(ref, sem.at[c], pl.ds(own + rows, size - rows) if c == near else pl.ds(start, size))

    sent(sx, s_x, (early, near, late))
    sent(sr, s_r, (early, near, late))
    sent(gs, s_g, (early, near))
    for c in (near, early):
        start, size = span[c]
        settle(gback, v_g.at[c], group_at(c))
        out = out + dot(comb[:, start:start + size], gback[group_at(c), :])
    plane_peers(lambda *a: gather(*a).wait_send())
    settle(gg_ref, v_sum.at[0], pl.ds(0, n))
    sent(gs, s_g, (late,))
    start, size = span[late]
    settle(gback, v_g.at[late], group_at(late))
    gx_ref[...] = (out + dot(comb[:, start:start + size], gback[group_at(late), :])).astype(BF16)


def solution(mesh):
    n = mesh.shape['ep']

    def layer_body(x_loc, r_loc, w_gate, w_in_loc, w_out_loc, first_ids, second_ids, keep_ids):
        groups, seq, hidden = x_loc.shape
        cap = 2 * seq // w_gate.shape[1]
        ff = w_in_loc.shape[2]
        tokens = groups * seq
        slots = n * groups * cap
        vmem = pl.BlockSpec(memory_space=pltpu.VMEM)
        hbm = pl.BlockSpec(memory_space=pltpu.HBM)
        dma = pltpu.SemaphoreType.DMA
        out = pl.pallas_call(
            functools.partial(layer_kernel, n, cap, seq),
            name='moe_layer',
            out_shape=(
                pltpu.VMEM((8, 128), F32),
                pltpu.VMEM((tokens, hidden), BF16),
                pltpu.VMEM((n, hidden), F32),
                pltpu.VMEM((hidden, ff), BF16),
                pltpu.VMEM((ff, hidden), BF16),
            ),
            in_specs=[hbm] * 8,
            out_specs=(vmem,) * 5,
            scratch_shapes=[
                pltpu.VMEM((groups, seq), jnp.int32),
                pltpu.VMEM((groups, seq), jnp.int32),
                pltpu.VMEM((groups, seq), jnp.int32),
                pltpu.VMEM((tokens, hidden), BF16),
                pltpu.VMEM((tokens, hidden), BF16),
                pltpu.VMEM((n, hidden), BF16),
                pltpu.VMEM((hidden, ff), BF16),
                pltpu.VMEM((ff, hidden), BF16),
                pltpu.VMEM((slots, hidden), BF16),
                pltpu.VMEM((slots, hidden), BF16),
                pltpu.VMEM((slots, hidden), BF16),
                pltpu.VMEM((slots, hidden), BF16),
                pltpu.VMEM((slots, hidden), BF16),
                pltpu.VMEM((slots, ff), BF16),
                pltpu.VMEM((slots, ff), BF16),
                pltpu.VMEM((slots, hidden), BF16),
                pltpu.VMEM((slots, hidden), BF16),
                pltpu.VMEM((n, 128), F32),
                pltpu.VMEM((n, 128), F32),
                pltpu.VMEM((n, 128), F32),
                pltpu.VMEM((n, 128), F32),
                pltpu.VMEM((n, hidden), F32),
                pltpu.VMEM((n, hidden), F32),
                pltpu.VMEM((8, hidden), F32),
                pltpu.VMEM((16, hidden), F32),
                pltpu.VMEM((8, hidden), F32),
                pltpu.VMEM((slots, ff), F32),
                pltpu.VMEM((slots, hidden), BF16),
                pltpu.VMEM((hidden, slots), BF16),
                dma((8,)),
                dma((3,)), dma((3,)), dma((3,)), dma((n,)), dma((n,)), dma((n,)), dma((16,)), dma((n,)),
                dma((3,)), dma((3,)), dma((3,)), dma((1,)), dma((1,)), dma((1,)), dma((1,)), dma((1,)),
            ],
            compiler_params=pltpu.CompilerParams(collective_id=0, has_side_effects=True, vmem_limit_bytes=44 * 1024 * 1024),
        )(*(pltpu.with_memory_space_constraint(a, pltpu.HBM) for a in (
            first_ids, second_ids, keep_ids, x_loc.reshape(tokens, hidden), r_loc.reshape(tokens, hidden), w_gate.T, w_in_loc[0], w_out_loc[0])))
        loss, gx, gg, gw1, gw2 = pl.pallas_call(
            write_kernel,
            name='write_results',
            out_shape=(
                jax.ShapeDtypeStruct((1, 1), F32),
                jax.ShapeDtypeStruct((tokens, hidden), BF16),
                jax.ShapeDtypeStruct((n, hidden), F32),
                jax.ShapeDtypeStruct((hidden, ff), BF16),
                jax.ShapeDtypeStruct((ff, hidden), BF16),
            ),
            in_specs=[vmem] * 5,
            out_specs=(pl.BlockSpec(memory_space=pltpu.SMEM), hbm, hbm, hbm, hbm),
            scratch_shapes=[dma((4,))],
            compiler_params=pltpu.CompilerParams(vmem_limit_bytes=2 * 1024 * 1024),
        )(*(pltpu.with_memory_space_constraint(a, pltpu.VMEM) for a in out))
        return loss.reshape(()), gx.reshape(x_loc.shape), gw1[None], gw2[None], gg.T

    row_spec = P('ep', None, None)
    id_spec = P('ep', None)
    return jax.shard_map(layer_body, mesh=mesh, in_specs=(row_spec, row_spec, P(None, None), row_spec, row_spec, id_spec, id_spec, id_spec), out_specs=(P(), row_spec, row_spec, row_spec, P(None, None)), check_vma=False)
```

```python
import functools

import jax
import jax.numpy as jnp
from jax import lax
from jax.experimental import pallas as pl
from jax.experimental.pallas import tpu as pltpu
from jax.sharding import PartitionSpec as P

ALPHA = 0.01
MESH = pl.DeviceIdType.MESH
F32 = jnp.float32
BF16 = jnp.bfloat16
NN = (((1,), (0,)), ((), ()))
NT = (((1,), (1,)), ((), ()))
TN = (((0,), (0,)), ((), ()))
GELU_C = 0.7978845608028654
GELU_K = 0.044715


def dot(a, b, dims=NN, **kw):
    return lax.dot_general(a, b, dims, preferred_element_type=F32, **kw)


def iota(shape, dim):
    return lax.broadcasted_iota(jnp.int32, shape, dim)


def flip_bits(a, b):
    return a + b - 2 * a * b


def write_kernel(loss_v, gx_v, gg_v, gw1_v, gw2_v, loss_s, gx_h, gg_h, gw1_h, gw2_h, sem):
    copies = [pltpu.make_async_copy(src, dst, sem.at[i]) for i, (src, dst) in enumerate(((gw1_v, gw1_h), (gw2_v, gw2_h), (gx_v, gx_h), (gg_v, gg_h)))]
    for copy in copies:
        copy.start()
    loss_s[0, 0] = jnp.max(loss_v[...])
    for copy in copies:
        copy.wait()


def layer_kernel(n, cap, seq, e1_hbm, e2_hbm, k2_hbm, x_hbm, r_hbm, wg_hbm, w1_hbm, w2_hbm,
                 loss_ref, gx_ref, gg_ref, gw1, gw2,
                 e1_ref, e2_ref, k2_ref, x_ref, r_ref, wg_ref, w1, w2, sx, sr, xe, re, gy, act, gpre, gs, gback,
                 rows_s, rows_r, dots_s, dots_r, part_s, part_r, mid_s, mid_r, sum_s, slope, hid, xet, in_sem,
                 s_x, s_r, s_g, s_row, s_dot, s_part, s_mid, s_sum,
                 v_x, v_r, v_g, v_row, v_dot, v_part, v_mid, v_sum):
    me = lax.axis_index('ep')
    tokens, hidden = x_ref.shape
    ff = w1.shape[1]
    groups = tokens // seq
    rows = groups * cap
    slots = n * rows
    plane = n // 4
    tokens_all = tokens * n
    numel = tokens_all * hidden

    low, high = lax.rem(me, plane), lax.div(me, plane)
    low_bits = [lax.rem(low, 2), lax.rem(lax.div(low, 2), 2), lax.div(low, 4)]
    high_bits = [lax.rem(high, 2), lax.div(high, 2)]
    order = (2, 0, 1, 3)
    own = plane * rows

    def partner(quarter, step):
        far = order[quarter]
        top = [bit if not (far >> i) & 1 else 1 - bit for i, bit in enumerate(high_bits)]
        step_bits = [lax.rem(step, 2), lax.rem(lax.div(step, 2), 2), lax.div(step, 4)]
        bits = [flip_bits(a, b) for a, b in zip(low_bits, step_bits)]
        return (top[0] + 2 * top[1]) * plane + bits[0] + 2 * bits[1] + 4 * bits[2]

    def each_partner(pieces, body):
        for quarter, lo, hi in pieces:
            first = max(lo, 1) if order[quarter] == 0 else lo

            @pl.loop(first, hi)
            def _(count):
                step = hi - 1 + first - count
                body(quarter * plane + step, partner(quarter, step))

    everyone = tuple((quarter, 0, plane) for quarter in (0, 3, 1, 2))
    early, near, late = 0, 1, 2
    quarters_of = (((0, 0, plane),), ((1, 0, plane), (2, 0, plane)), ((3, 0, plane),))
    span = ((0, plane * rows), (plane * rows, 2 * plane * rows), (3 * plane * rows, plane * rows))

    barrier = pltpu.get_barrier_semaphore()
    each_partner(everyone, lambda q, d: pl.semaphore_signal(barrier, inc=1, device_id=(d,), device_id_type=MESH))
    fetched = [pltpu.make_async_copy(src, dst, in_sem.at[i]) for i, (src, dst) in enumerate((
        (e1_hbm, e1_ref), (e2_hbm, e2_ref), (k2_hbm, k2_ref), (x_hbm, x_ref), (r_hbm, r_ref), (wg_hbm, wg_ref), (w1_hbm, w1), (w2_hbm, w2)))]
    for copy in fetched:
        copy.start()
    for copy in fetched[:3]:
        copy.wait()

    spread = (iota((seq, tokens), 1) % seq == iota((seq, tokens), 0)).astype(F32).astype(BF16)
    own_group = iota((groups, tokens), 1) // seq == iota((groups, tokens), 0)

    def along_lanes(ref):
        wide = dot(ref[...].astype(F32).astype(BF16), spread)
        return jnp.sum(jnp.where(own_group, wide, 0.0), axis=0, keepdims=True).astype(jnp.int32)

    e1, e2, k2 = along_lanes(e1_ref), along_lanes(e2_ref), along_lanes(k2_ref)
    row_i, col_i = iota((tokens, tokens), 0), iota((tokens, tokens), 1)
    eye = row_i == col_i

    def column(row):
        return jnp.sum(jnp.where(eye, row, 0), axis=1, keepdims=True)

    e1c, e2c, k2c = column(e1), column(e2), column(k2)
    same_group = (row_i // seq) == (col_i // seq)
    earlier = same_group & (row_i < col_i)
    one = jnp.int32(1)
    pos1 = jnp.sum(jnp.where(earlier & (e1c == e1), one, 0), axis=0, keepdims=True)
    count1 = jnp.sum(jnp.where(same_group & (e1c == e2), one, 0), axis=0, keepdims=True)
    before2 = jnp.sum(jnp.where(earlier & (e2c == e2) & (k2c > 0), one, 0), axis=0, keepdims=True)
    pos2 = count1 + before2
    lane = iota((1, tokens), 1)
    group_base = (lane // seq) * cap
    kept1 = pos1 < cap
    kept2 = (pos2 < cap) & (k2 > 0)
    place1 = jnp.where(kept1, group_base + pos1, -1)
    place2 = jnp.where(kept2, group_base + pos2, -1)

    def slot_of(expert):
        apart = expert ^ me
        top = apart // plane
        quarter = jnp.where(top == order[0], 0, jnp.where(top == order[3], 3, top + 1))
        return quarter * plane + apart % plane

    key1 = jnp.where(kept1, slot_of(e1) * rows + place1, -1)
    key2 = jnp.where(kept2, slot_of(e2) * rows + place2, -1)
    slot_i = iota((slots, tokens), 0)
    disp = ((slot_i == key1) | (slot_i == key2)).astype(F32).astype(BF16)

    fetched[3].wait()
    x = x_ref[...]
    first_rows = plane * rows
    sx[0:first_rows, :] = dot(disp[0:first_rows], x).astype(BF16)

    pl.semaphore_wait(barrier, n - 1)

    def one_row(src, dst, src_row, send, recv, q, d):
        return pltpu.make_async_remote_copy(src.at[pl.ds(src_row, 1)], dst.at[pl.ds(me, 1)], send.at[q], recv.at[0], device_id=(d,), device_id_type=MESH)

    def block(src, dst, send, recv, half_i, q, d):
        at = pl.ds(q * rows, rows)
        return pltpu.make_async_remote_copy(src.at[at], dst.at[at], send.at[half_i], recv.at[half_i], device_id=(d,), device_id_type=MESH)

    def own_row(src, dst, src_row, recv):
        pltpu.make_async_copy(src.at[pl.ds(src_row, 1)], dst.at[pl.ds(me, 1)], recv.at[0]).start()

    def own_block(src, dst, recv):
        pltpu.make_async_copy(src.at[pl.ds(own, rows)], dst.at[pl.ds(own, rows)], recv.at[near]).start()

    def settle(ref, sem, rows_at):
        pltpu.make_async_copy(ref.at[rows_at], ref.at[rows_at], sem).wait()

    def group_at(c):
        return pl.ds(*span[c])

    def send_group(src, dst, send, recv, c, pieces=None):
        each_partner(pieces or quarters_of[c], lambda q, d: block(src, dst, send, recv, c, q, d).start())

    send_group(sx, xe, s_x, v_x, early)
    sx[first_rows:, :] = dot(disp[first_rows:], x).astype(BF16)
    send_group(sx, xe, s_x, v_x, near)
    own_block(sx, xe, v_x)
    fetched[4].wait()
    fetched[5].wait()

    expert_i = iota((n, tokens), 0)
    hot1 = (expert_i == e1).astype(F32)
    hot2 = (expert_i == e2).astype(F32)
    place_i = iota((128, tokens), 0)
    at1 = (place_i == place1).astype(F32)
    at2 = (place_i == place2).astype(F32)

    wgt = wg_ref[...]
    logits = dot(wgt, x, NT)
    top_logit = jnp.max(logits, axis=0, keepdims=True)
    expd = jnp.exp(logits - top_logit)
    prob = expd / jnp.sum(expd, axis=0, keepdims=True)
    g1 = jnp.sum(prob * hot1, axis=0, keepdims=True)
    g2 = jnp.sum(prob * hot2, axis=0, keepdims=True)
    gsum = g1 + g2
    ratio1, ratio2 = g1 / gsum, g2 / gsum
    n1 = ratio1.astype(BF16).astype(F32)
    n2 = ratio2.astype(BF16).astype(F32)
    mix = ratio1 * ratio2
    exact = lax.Precision.HIGHEST
    expert_f = expert_i.astype(F32)
    e1f, e2f = jnp.sum(hot1 * expert_f, axis=0, keepdims=True), jnp.sum(hot2 * expert_f, axis=0, keepdims=True)

    def placed(place, base):
        return (place_i == jnp.where(place >= 0, place + base, -1)).astype(F32)

    norm_rows = dot(hot1 * n1, at1, NT, precision=exact) + dot(hot2 * n2, at2, NT, precision=exact)
    norm_rows = norm_rows + dot(hot1 * mix, placed(place1, 16), NT, precision=exact) + dot(hot2 * mix, placed(place2, 16), NT, precision=exact)
    norm_rows = norm_rows + dot(hot1 * e2f, placed(place1, 104), NT, precision=exact) + dot(hot2 * e1f, placed(place2, 104), NT, precision=exact)
    sub_n, lane_n = iota((n, 128), 0), iota((n, 128), 1)

    def as_lanes(col, base):
        return jnp.sum(jnp.where(lane_n == sub_n + base, col, 0.0), axis=0, keepdims=True)

    def as_column(row, base):
        return jnp.sum(jnp.where(lane_n == sub_n + base, row, 0.0), axis=1, keepdims=True)

    r = r_ref[...]
    xr = jnp.sum(jnp.sum(x.astype(F32) * r.astype(F32), axis=0, keepdims=True), axis=1, keepdims=True)
    lane_1 = iota((1, 128), 1)
    stats = as_lanes(jnp.sum(hot1, axis=1, keepdims=True), 32) + as_lanes(jnp.sum(prob, axis=1, keepdims=True), 64) + jnp.where(lane_1 == 96, xr, 0.0)
    rows_s[...] = norm_rows + stats

    sr[...] = dot(disp, r).astype(BF16)
    each_partner(everyone, lambda q, d: one_row(rows_s, rows_r, d, s_row, v_row, q, d).start())
    own_row(rows_s, rows_r, me, v_row)
    send_group(sr, re, s_r, v_r, early)
    send_group(sx, xe, s_x, v_x, late)
    send_group(sr, re, s_r, v_r, near)
    own_block(sr, re, v_r)
    send_group(sr, re, s_r, v_r, late)

    slot_row = iota((slots, n), 0)
    quarter = slot_row // rows // plane
    far = jnp.where(quarter == 0, order[0], jnp.where(quarter == 3, order[3], quarter - 1))
    source = (far * plane + slot_row // rows % plane) ^ me
    pick = (source == iota((slots, n), 1)).astype(F32)
    lane_s, row_s = iota((slots, 128), 1), iota((slots, 128), 0) % rows
    mine = lane_s == row_s
    key1c, key2c = column(key1), column(key2)
    slot_l = iota((tokens, slots), 1)
    comb = ((slot_l == key1c) | (slot_l == key2c)).astype(F32).astype(BF16)
    fetched[6].wait()
    fetched[7].wait()

    def forward(c):
        at = group_at(c)
        settle(xe, v_x.at[c], at)
        pre = dot(xe[at, :], w1[...])
        sq = pre * pre
        th = jnp.tanh(GELU_C * (pre + GELU_K * (sq * pre)))
        cdf = 0.5 * (1.0 + th)
        slope[at, :] = cdf + (0.5 * GELU_C) * pre * (1.0 - th * th) * (1.0 + 3 * GELU_K * sq)
        act[at, :] = (pre * cdf).astype(BF16)
        hid[at, :] = dot(act[at, :], w2[...]).astype(BF16)

    def receive(c):
        at = group_at(c)
        start, size = span[c]
        settle(re, v_r.at[c], at)
        rc = re[at, :].astype(F32)
        norm = norms[start:start + size]
        gy[at, :] = (norm * rc).astype(BF16)
        d = jnp.sum(hid[at, :].astype(F32) * rc, axis=1, keepdims=True)
        share = mixes[start:start + size] * d.astype(BF16).astype(F32) * signs[start:start + size]
        part_s[...] += dot(share.astype(BF16), xe[at, :], TN)
        in_lane = jnp.where(mine[start:start + size], d, 0.0)
        dots_s[pl.ds(start // rows, size // rows), :] = jnp.sum(in_lane.reshape(size // rows, rows, 128), axis=1)
        return jnp.sum(norm * d, axis=0, keepdims=True)

    def backward(c):
        at = group_at(c)
        ga = dot(gy[at, :], w2[...], NT).astype(BF16)
        gpre[at, :] = (ga.astype(F32) * slope[at, :]).astype(BF16)
        gs[at, :] = dot(gpre[at, :], w1[...], NT).astype(BF16)

    def send_back(c, pieces=None):
        send_group(gs, gback, s_g, v_g, c, pieces)

    forward(early)
    forward(near)
    settle(rows_r, v_row.at[0], pl.ds(0, n))
    all_rows = rows_r[...]
    total = jnp.sum(all_rows, axis=0, keepdims=True)
    frac = as_column(total, 32) / tokens_all
    mean_prob = as_column(total, 64) / tokens_all
    wide = dot(pick, all_rows, precision=exact)
    norms = jnp.sum(jnp.where(mine, wide, 0.0), axis=1, keepdims=True)
    mixes = jnp.sum(jnp.where(lane_s == row_s + 16, wide, 0.0), axis=1, keepdims=True)
    others = jnp.sum(jnp.where(lane_s == row_s + 104, wide, 0.0), axis=1, keepdims=True)
    column_i = iota((slots, n), 1)
    signs = (column_i == me).astype(F32) - (column_i.astype(F32) == others).astype(F32)
    aux_prob = (ALPHA * hidden * n) * frac
    aux_log = prob * (aux_prob - jnp.sum(prob * aux_prob, axis=0, keepdims=True))
    part_s[...] = dot(aux_log.astype(BF16), x_ref[...])

    loss_part = receive(early)
    backward(early)
    split_late = 1
    send_back(early)
    loss_part = loss_part + receive(near)
    backward(near)
    send_back(near)
    own_block(gs, gback, v_g)
    forward(late)
    xet[...] = jnp.transpose(xe[...])
    loss_part = loss_part + receive(late)
    dots_s[...] = dots_s[...] + jnp.where(lane_1 == 16, loss_part, 0.0)

    share_rows = n // plane

    def line_copy(src, src_row, dst, dst_row, send, recv, q, d):
        return pltpu.make_async_remote_copy(src.at[pl.ds(src_row, 1)], dst.at[pl.ds(dst_row, 1)], send.at[q], recv.at[0], device_id=(d,), device_id_type=MESH)

    def own_line(src, src_row, dst, dst_row, recv):
        pltpu.make_async_copy(src.at[pl.ds(src_row, 1)], dst.at[pl.ds(dst_row, 1)], recv.at[0]).start()

    def plane_peers(body):
        @pl.loop(1, plane)
        def _(step):
            d = partner(1, step)
            for j in range(share_rows):
                body(step * share_rows + j, d, lax.rem(d, plane) * share_rows + j, low * share_rows + j, j)

    def scatter(q, d, theirs, ours, j):
        return line_copy(part_s, theirs, part_r, ours, s_part, v_part, q, d)

    def line_peers(body):
        for quarter in (0, 3, 2):
            d = partner(quarter, 0)
            for j in range(share_rows):
                body(quarter * share_rows + j, d, j)

    def exchange(q, d, j):
        return line_copy(mid_s, j, mid_r, high * share_rows + j, s_mid, v_mid, q, d)

    def gather(q, d, theirs, ours, j):
        return line_copy(sum_s, j, gg_ref, ours, s_sum, v_sum, q, d)

    plane_peers(lambda *a: scatter(*a).start())
    for j in range(share_rows):
        own_line(part_s, low * share_rows + j, part_r, low * share_rows + j, v_part)
    backward(late)
    send_back(late, ((3, plane - split_late, plane),))
    settle(part_r, v_part.at[0], pl.ds(0, n))
    fold = part_r[0:8, :] + part_r[8:16, :] + part_r[16:24, :] + part_r[24:32, :]
    mid_s[0:4, :] = fold[0:4] + fold[4:8]
    line_peers(lambda *a: exchange(*a).start())
    for j in range(share_rows):
        own_line(mid_s, j, mid_r, high * share_rows + j, v_mid)
    each_partner(everyone, lambda q, d: one_row(dots_s, dots_r, q, s_dot, v_dot, q, d).start())
    own_row(dots_s, dots_r, plane, v_dot)
    send_back(late, ((3, 0, plane - split_late),))
    gw1[...] = dot(xet[...], gpre[...]).astype(BF16)
    gw2[...] = dot(act[...], gy[...], TN).astype(BF16)

    settle(mid_r, v_mid.at[0], pl.ds(0, 16))
    fold = mid_r[0:8, :] + mid_r[8:16, :]
    sum_s[0:4, :] = fold[0:4] + fold[4:8]
    plane_peers(lambda *a: gather(*a).start())
    for j in range(share_rows):
        own_line(sum_s, j, gg_ref, low * share_rows + j, v_sum)

    settle(dots_r, v_dot.at[0], pl.ds(0, n))
    all_dots = dots_r[...]
    d1 = jnp.sum(dot(all_dots, hot1, TN, precision=exact) * at1, axis=0, keepdims=True)
    d2 = jnp.sum(dot(all_dots, hot2, TN, precision=exact) * at2, axis=0, keepdims=True)
    apart = d1.astype(BF16).astype(F32) - d2.astype(BF16).astype(F32)
    glog = (aux_log + (mix * apart) * (hot1 - hot2)).astype(BF16)

    both = jnp.sum(jnp.where(lane_1 == 96, total, 0.0), axis=1, keepdims=True)
    both = both + jnp.sum(jnp.where(lane_1 == 16, jnp.sum(all_dots, axis=0, keepdims=True), 0.0), axis=1, keepdims=True)
    aux = jnp.sum(frac * mean_prob, axis=0, keepdims=True) * n
    loss_ref[...] = jnp.broadcast_to(both / numel + ALPHA * aux, loss_ref.shape)
    out = r_ref[...].astype(F32) + dot(glog, wg_ref[...], TN)
    each_partner(everyone, lambda q, d: one_row(rows_s, rows_r, d, s_row, v_row, q, d).wait_send())
    each_partner(everyone, lambda q, d: one_row(dots_s, dots_r, q, s_dot, v_dot, q, d).wait_send())
    plane_peers(lambda *a: scatter(*a).wait_send())
    line_peers(lambda *a: exchange(*a).wait_send())

    def sent(ref, sem, groups_sent):
        for c in groups_sent:
            start, size = span[c]
            settle(ref, sem.at[c], pl.ds(own + rows, size - rows) if c == near else pl.ds(start, size))

    sent(sx, s_x, (early, near, late))
    sent(sr, s_r, (early, near, late))
    sent(gs, s_g, (early, near))
    for c in (near, early):
        start, size = span[c]
        settle(gback, v_g.at[c], group_at(c))
        out = out + dot(comb[:, start:start + size], gback[group_at(c), :])
    plane_peers(lambda *a: gather(*a).wait_send())
    settle(gg_ref, v_sum.at[0], pl.ds(0, n))
    sent(gs, s_g, (late,))
    start, size = span[late]
    settle(gback, v_g.at[late], group_at(late))
    gx_ref[...] = (out + dot(comb[:, start:start + size], gback[group_at(late), :])).astype(BF16)


def solution(mesh):
    n = mesh.shape['ep']

    def layer_body(x_loc, r_loc, w_gate, w_in_loc, w_out_loc, first_ids, second_ids, keep_ids):
        groups, seq, hidden = x_loc.shape
        cap = 2 * seq // w_gate.shape[1]
        ff = w_in_loc.shape[2]
        tokens = groups * seq
        slots = n * groups * cap
        vmem = pl.BlockSpec(memory_space=pltpu.VMEM)
        hbm = pl.BlockSpec(memory_space=pltpu.HBM)
        dma = pltpu.SemaphoreType.DMA
        out = pl.pallas_call(
            functools.partial(layer_kernel, n, cap, seq),
            name='moe_layer',
            out_shape=(
                pltpu.VMEM((8, 128), F32),
                pltpu.VMEM((tokens, hidden), BF16),
                pltpu.VMEM((n, hidden), F32),
                pltpu.VMEM((hidden, ff), BF16),
                pltpu.VMEM((ff, hidden), BF16),
            ),
            in_specs=[hbm] * 8,
            out_specs=(vmem,) * 5,
            scratch_shapes=[
                pltpu.VMEM((groups, seq), jnp.int32),
                pltpu.VMEM((groups, seq), jnp.int32),
                pltpu.VMEM((groups, seq), jnp.int32),
                pltpu.VMEM((tokens, hidden), BF16),
                pltpu.VMEM((tokens, hidden), BF16),
                pltpu.VMEM((n, hidden), BF16),
                pltpu.VMEM((hidden, ff), BF16),
                pltpu.VMEM((ff, hidden), BF16),
                pltpu.VMEM((slots, hidden), BF16),
                pltpu.VMEM((slots, hidden), BF16),
                pltpu.VMEM((slots, hidden), BF16),
                pltpu.VMEM((slots, hidden), BF16),
                pltpu.VMEM((slots, hidden), BF16),
                pltpu.VMEM((slots, ff), BF16),
                pltpu.VMEM((slots, ff), BF16),
                pltpu.VMEM((slots, hidden), BF16),
                pltpu.VMEM((slots, hidden), BF16),
                pltpu.VMEM((n, 128), F32),
                pltpu.VMEM((n, 128), F32),
                pltpu.VMEM((n, 128), F32),
                pltpu.VMEM((n, 128), F32),
                pltpu.VMEM((n, hidden), F32),
                pltpu.VMEM((n, hidden), F32),
                pltpu.VMEM((8, hidden), F32),
                pltpu.VMEM((16, hidden), F32),
                pltpu.VMEM((8, hidden), F32),
                pltpu.VMEM((slots, ff), F32),
                pltpu.VMEM((slots, hidden), BF16),
                pltpu.VMEM((hidden, slots), BF16),
                dma((8,)),
                dma((3,)), dma((3,)), dma((3,)), dma((n,)), dma((n,)), dma((n,)), dma((16,)), dma((n,)),
                dma((3,)), dma((3,)), dma((3,)), dma((1,)), dma((1,)), dma((1,)), dma((1,)), dma((1,)),
            ],
            compiler_params=pltpu.CompilerParams(collective_id=0, has_side_effects=True, vmem_limit_bytes=44 * 1024 * 1024),
        )(*(pltpu.with_memory_space_constraint(a, pltpu.HBM) for a in (
            first_ids, second_ids, keep_ids, x_loc.reshape(tokens, hidden), r_loc.reshape(tokens, hidden), w_gate.T, w_in_loc[0], w_out_loc[0])))
        loss, gx, gg, gw1, gw2 = pl.pallas_call(
            write_kernel,
            name='write_results',
            out_shape=(
                jax.ShapeDtypeStruct((1, 1), F32),
                jax.ShapeDtypeStruct((tokens, hidden), BF16),
                jax.ShapeDtypeStruct((n, hidden), F32),
                jax.ShapeDtypeStruct((hidden, ff), BF16),
                jax.ShapeDtypeStruct((ff, hidden), BF16),
            ),
            in_specs=[vmem] * 5,
            out_specs=(pl.BlockSpec(memory_space=pltpu.SMEM), hbm, hbm, hbm, hbm),
            scratch_shapes=[dma((4,))],
            compiler_params=pltpu.CompilerParams(vmem_limit_bytes=2 * 1024 * 1024),
        )(*(pltpu.with_memory_space_constraint(a, pltpu.VMEM) for a in out))
        return loss.reshape(()), gx.reshape(x_loc.shape), gw1[None], gw2[None], gg.T

    row_spec = P('ep', None, None)
    id_spec = P('ep', None)
    return jax.shard_map(layer_body, mesh=mesh, in_specs=(row_spec, row_spec, P(None, None), row_spec, row_spec, id_spec, id_spec, id_spec), out_specs=(P(), row_spec, row_spec, row_spec, P(None, None)), check_vma=False)
```

```python
import functools

import jax
import jax.numpy as jnp
from jax import lax
from jax.experimental import pallas as pl
from jax.experimental.pallas import tpu as pltpu
from jax.sharding import PartitionSpec as P

ALPHA = 0.01
MESH = pl.DeviceIdType.MESH
F32 = jnp.float32
BF16 = jnp.bfloat16
NN = (((1,), (0,)), ((), ()))
NT = (((1,), (1,)), ((), ()))
TN = (((0,), (0,)), ((), ()))
GELU_C = 0.7978845608028654
GELU_K = 0.044715


def dot(a, b, dims=NN, **kw):
    return lax.dot_general(a, b, dims, preferred_element_type=F32, **kw)


def iota(shape, dim):
    return lax.broadcasted_iota(jnp.int32, shape, dim)


def flip_bits(a, b):
    return a + b - 2 * a * b


def write_kernel(loss_v, gx_v, gg_v, gw1_v, gw2_v, loss_s, gx_h, gg_h, gw1_h, gw2_h, sem):
    copies = [pltpu.make_async_copy(src, dst, sem.at[i]) for i, (src, dst) in enumerate(((gw1_v, gw1_h), (gw2_v, gw2_h), (gx_v, gx_h), (gg_v, gg_h)))]
    for copy in copies:
        copy.start()
    loss_s[0, 0] = jnp.max(loss_v[...])
    for copy in copies:
        copy.wait()


def layer_kernel(n, cap, seq, e1_hbm, e2_hbm, k2_hbm, x_hbm, r_hbm, wg_hbm, w1_hbm, w2_hbm,
                 loss_ref, gx_ref, gg_ref, gw1, gw2,
                 e1_ref, e2_ref, k2_ref, x_ref, r_ref, wg_ref, w1, w2, sx, sr, xe, re, gy, act, gpre, gs, gback,
                 rows_s, rows_r, dots_s, dots_r, part_s, part_r, mid_s, mid_r, sum_s, slope, hid, xet, in_sem,
                 s_x, s_r, s_g, s_row, s_dot, s_part, s_mid, s_sum,
                 v_x, v_r, v_g, v_row, v_dot, v_part, v_mid, v_sum):
    me = lax.axis_index('ep')
    tokens, hidden = x_ref.shape
    ff = w1.shape[1]
    groups = tokens // seq
    rows = groups * cap
    slots = n * rows
    plane = n // 4
    tokens_all = tokens * n
    numel = tokens_all * hidden

    low, high = lax.rem(me, plane), lax.div(me, plane)
    low_bits = [lax.rem(low, 2), lax.rem(lax.div(low, 2), 2), lax.div(low, 4)]
    high_bits = [lax.rem(high, 2), lax.div(high, 2)]
    order = (2, 0, 1, 3)
    own = plane * rows

    def partner(quarter, step):
        far = order[quarter]
        top = [bit if not (far >> i) & 1 else 1 - bit for i, bit in enumerate(high_bits)]
        step_bits = [lax.rem(step, 2), lax.rem(lax.div(step, 2), 2), lax.div(step, 4)]
        bits = [flip_bits(a, b) for a, b in zip(low_bits, step_bits)]
        return (top[0] + 2 * top[1]) * plane + bits[0] + 2 * bits[1] + 4 * bits[2]

    def each_partner(pieces, body):
        for quarter, lo, hi in pieces:
            first = max(lo, 1) if order[quarter] == 0 else lo

            @pl.loop(first, hi)
            def _(count):
                step = hi - 1 + first - count
                body(quarter * plane + step, partner(quarter, step))

    everyone = tuple((quarter, 0, plane) for quarter in (0, 3, 1, 2))
    early, near, late = 0, 1, 2
    quarters_of = (((0, 0, plane),), ((1, 0, plane), (2, 0, plane)), ((3, 0, plane),))
    span = ((0, plane * rows), (plane * rows, 2 * plane * rows), (3 * plane * rows, plane * rows))

    barrier = pltpu.get_barrier_semaphore()
    each_partner(everyone, lambda q, d: pl.semaphore_signal(barrier, inc=1, device_id=(d,), device_id_type=MESH))
    fetched = [pltpu.make_async_copy(src, dst, in_sem.at[i]) for i, (src, dst) in enumerate((
        (e1_hbm, e1_ref), (e2_hbm, e2_ref), (k2_hbm, k2_ref), (x_hbm, x_ref), (r_hbm, r_ref), (wg_hbm, wg_ref), (w1_hbm, w1), (w2_hbm, w2)))]
    for copy in fetched:
        copy.start()
    for copy in fetched[:3]:
        copy.wait()

    spread = (iota((seq, tokens), 1) % seq == iota((seq, tokens), 0)).astype(F32).astype(BF16)
    own_group = iota((groups, tokens), 1) // seq == iota((groups, tokens), 0)

    def along_lanes(ref):
        wide = dot(ref[...].astype(F32).astype(BF16), spread)
        return jnp.sum(jnp.where(own_group, wide, 0.0), axis=0, keepdims=True).astype(jnp.int32)

    e1, e2, k2 = along_lanes(e1_ref), along_lanes(e2_ref), along_lanes(k2_ref)
    row_i, col_i = iota((tokens, tokens), 0), iota((tokens, tokens), 1)
    eye = row_i == col_i

    def column(row):
        return jnp.sum(jnp.where(eye, row, 0), axis=1, keepdims=True)

    e1c, e2c, k2c = column(e1), column(e2), column(k2)
    same_group = (row_i // seq) == (col_i // seq)
    earlier = same_group & (row_i < col_i)
    one = jnp.int32(1)
    pos1 = jnp.sum(jnp.where(earlier & (e1c == e1), one, 0), axis=0, keepdims=True)
    count1 = jnp.sum(jnp.where(same_group & (e1c == e2), one, 0), axis=0, keepdims=True)
    before2 = jnp.sum(jnp.where(earlier & (e2c == e2) & (k2c > 0), one, 0), axis=0, keepdims=True)
    pos2 = count1 + before2
    lane = iota((1, tokens), 1)
    group_base = (lane // seq) * cap
    kept1 = pos1 < cap
    kept2 = (pos2 < cap) & (k2 > 0)
    place1 = jnp.where(kept1, group_base + pos1, -1)
    place2 = jnp.where(kept2, group_base + pos2, -1)

    def slot_of(expert):
        apart = expert ^ me
        top = apart // plane
        quarter = jnp.where(top == order[0], 0, jnp.where(top == order[3], 3, top + 1))
        return quarter * plane + apart % plane

    key1 = jnp.where(kept1, slot_of(e1) * rows + place1, -1)
    key2 = jnp.where(kept2, slot_of(e2) * rows + place2, -1)
    slot_i = iota((slots, tokens), 0)
    disp = ((slot_i == key1) | (slot_i == key2)).astype(F32).astype(BF16)

    fetched[3].wait()
    x = x_ref[...]
    first_rows = plane * rows
    sx[0:first_rows, :] = dot(disp[0:first_rows], x).astype(BF16)

    pl.semaphore_wait(barrier, n - 1)

    def one_row(src, dst, src_row, send, recv, q, d):
        return pltpu.make_async_remote_copy(src.at[pl.ds(src_row, 1)], dst.at[pl.ds(me, 1)], send.at[q], recv.at[0], device_id=(d,), device_id_type=MESH)

    def block(src, dst, send, recv, half_i, q, d):
        at = pl.ds(q * rows, rows)
        return pltpu.make_async_remote_copy(src.at[at], dst.at[at], send.at[half_i], recv.at[half_i], device_id=(d,), device_id_type=MESH)

    def own_row(src, dst, src_row, recv):
        pltpu.make_async_copy(src.at[pl.ds(src_row, 1)], dst.at[pl.ds(me, 1)], recv.at[0]).start()

    def own_block(src, dst, recv):
        pltpu.make_async_copy(src.at[pl.ds(own, rows)], dst.at[pl.ds(own, rows)], recv.at[near]).start()

    def settle(ref, sem, rows_at):
        pltpu.make_async_copy(ref.at[rows_at], ref.at[rows_at], sem).wait()

    def group_at(c):
        return pl.ds(*span[c])

    def send_group(src, dst, send, recv, c, pieces=None):
        each_partner(pieces or quarters_of[c], lambda q, d: block(src, dst, send, recv, c, q, d).start())

    send_group(sx, xe, s_x, v_x, early)
    sx[first_rows:, :] = dot(disp[first_rows:], x).astype(BF16)
    send_group(sx, xe, s_x, v_x, near)
    own_block(sx, xe, v_x)
    fetched[4].wait()
    fetched[5].wait()

    expert_i = iota((n, tokens), 0)
    hot1 = (expert_i == e1).astype(F32)
    hot2 = (expert_i == e2).astype(F32)
    place_i = iota((128, tokens), 0)
    at1 = (place_i == place1).astype(F32)
    at2 = (place_i == place2).astype(F32)

    wgt = wg_ref[...]
    logits = dot(wgt, x, NT)
    top_logit = jnp.max(logits, axis=0, keepdims=True)
    expd = jnp.exp(logits - top_logit)
    prob = expd / jnp.sum(expd, axis=0, keepdims=True)
    g1 = jnp.sum(prob * hot1, axis=0, keepdims=True)
    g2 = jnp.sum(prob * hot2, axis=0, keepdims=True)
    gsum = g1 + g2
    ratio1, ratio2 = g1 / gsum, g2 / gsum
    n1 = ratio1.astype(BF16).astype(F32)
    n2 = ratio2.astype(BF16).astype(F32)
    mix = ratio1 * ratio2
    exact = lax.Precision.HIGHEST
    expert_f = expert_i.astype(F32)
    e1f, e2f = jnp.sum(hot1 * expert_f, axis=0, keepdims=True), jnp.sum(hot2 * expert_f, axis=0, keepdims=True)

    def placed(place, base):
        return (place_i == jnp.where(place >= 0, place + base, -1)).astype(F32)

    norm_rows = dot(hot1 * n1, at1, NT, precision=exact) + dot(hot2 * n2, at2, NT, precision=exact)
    norm_rows = norm_rows + dot(hot1 * mix, placed(place1, 16), NT, precision=exact) + dot(hot2 * mix, placed(place2, 16), NT, precision=exact)
    norm_rows = norm_rows + dot(hot1 * e2f, placed(place1, 104), NT, precision=exact) + dot(hot2 * e1f, placed(place2, 104), NT, precision=exact)
    sub_n, lane_n = iota((n, 128), 0), iota((n, 128), 1)

    def as_lanes(col, base):
        return jnp.sum(jnp.where(lane_n == sub_n + base, col, 0.0), axis=0, keepdims=True)

    def as_column(row, base):
        return jnp.sum(jnp.where(lane_n == sub_n + base, row, 0.0), axis=1, keepdims=True)

    r = r_ref[...]
    xr = jnp.sum(jnp.sum(x.astype(F32) * r.astype(F32), axis=0, keepdims=True), axis=1, keepdims=True)
    lane_1 = iota((1, 128), 1)
    stats = as_lanes(jnp.sum(hot1, axis=1, keepdims=True), 32) + as_lanes(jnp.sum(prob, axis=1, keepdims=True), 64) + jnp.where(lane_1 == 96, xr, 0.0)
    rows_s[...] = norm_rows + stats

    sr[...] = dot(disp, r).astype(BF16)
    each_partner(everyone, lambda q, d: one_row(rows_s, rows_r, d, s_row, v_row, q, d).start())
    own_row(rows_s, rows_r, me, v_row)
    send_group(sr, re, s_r, v_r, early)
    send_group(sx, xe, s_x, v_x, late)
    send_group(sr, re, s_r, v_r, near)
    own_block(sr, re, v_r)
    send_group(sr, re, s_r, v_r, late)

    slot_row = iota((slots, n), 0)
    quarter = slot_row // rows // plane
    far = jnp.where(quarter == 0, order[0], jnp.where(quarter == 3, order[3], quarter - 1))
    source = (far * plane + slot_row // rows % plane) ^ me
    pick = (source == iota((slots, n), 1)).astype(F32)
    lane_s, row_s = iota((slots, 128), 1), iota((slots, 128), 0) % rows
    mine = lane_s == row_s
    key1c, key2c = column(key1), column(key2)
    slot_l = iota((tokens, slots), 1)
    comb = ((slot_l == key1c) | (slot_l == key2c)).astype(F32).astype(BF16)
    fetched[6].wait()
    fetched[7].wait()

    def forward(c):
        at = group_at(c)
        settle(xe, v_x.at[c], at)
        pre = dot(xe[at, :], w1[...])
        sq = pre * pre
        th = jnp.tanh(GELU_C * (pre + GELU_K * (sq * pre)))
        cdf = 0.5 * (1.0 + th)
        slope[at, :] = cdf + (0.5 * GELU_C) * pre * (1.0 - th * th) * (1.0 + 3 * GELU_K * sq)
        act[at, :] = (pre * cdf).astype(BF16)
        hid[at, :] = dot(act[at, :], w2[...]).astype(BF16)

    def receive(c):
        at = group_at(c)
        start, size = span[c]
        settle(re, v_r.at[c], at)
        rc = re[at, :].astype(F32)
        norm = norms[start:start + size]
        gy[at, :] = (norm * rc).astype(BF16)
        d = jnp.sum(hid[at, :].astype(F32) * rc, axis=1, keepdims=True)
        share = mixes[start:start + size] * d.astype(BF16).astype(F32) * signs[start:start + size]
        part_s[...] += dot(share.astype(BF16), xe[at, :], TN)
        in_lane = jnp.where(mine[start:start + size], d, 0.0)
        dots_s[pl.ds(start // rows, size // rows), :] = jnp.sum(in_lane.reshape(size // rows, rows, 128), axis=1)
        return jnp.sum(norm * d, axis=0, keepdims=True)

    def backward(c):
        at = group_at(c)
        ga = dot(gy[at, :], w2[...], NT).astype(BF16)
        gpre[at, :] = (ga.astype(F32) * slope[at, :]).astype(BF16)
        gs[at, :] = dot(gpre[at, :], w1[...], NT).astype(BF16)

    def send_back(c, pieces=None):
        send_group(gs, gback, s_g, v_g, c, pieces)

    forward(early)
    forward(near)
    settle(rows_r, v_row.at[0], pl.ds(0, n))
    all_rows = rows_r[...]
    total = jnp.sum(all_rows, axis=0, keepdims=True)
    frac = as_column(total, 32) / tokens_all
    mean_prob = as_column(total, 64) / tokens_all
    wide = dot(pick, all_rows, precision=exact)
    norms = jnp.sum(jnp.where(mine, wide, 0.0), axis=1, keepdims=True)
    mixes = jnp.sum(jnp.where(lane_s == row_s + 16, wide, 0.0), axis=1, keepdims=True)
    others = jnp.sum(jnp.where(lane_s == row_s + 104, wide, 0.0), axis=1, keepdims=True)
    column_i = iota((slots, n), 1)
    signs = (column_i == me).astype(F32) - (column_i.astype(F32) == others).astype(F32)
    aux_prob = (ALPHA * hidden * n) * frac
    aux_log = prob * (aux_prob - jnp.sum(prob * aux_prob, axis=0, keepdims=True))
    part_s[...] = dot(aux_log.astype(BF16), x_ref[...])

    loss_part = receive(early)
    backward(early)
    send_back(early)
    loss_part = loss_part + receive(near)
    backward(near)
    send_back(near)
    own_block(gs, gback, v_g)
    forward(late)
    xet[...] = jnp.transpose(xe[...])
    loss_part = loss_part + receive(late)
    dots_s[...] = dots_s[...] + jnp.where(lane_1 == 16, loss_part, 0.0)

    share_rows = n // plane

    def line_copy(src, src_row, dst, dst_row, send, recv, q, d):
        return pltpu.make_async_remote_copy(src.at[pl.ds(src_row, 1)], dst.at[pl.ds(dst_row, 1)], send.at[q], recv.at[0], device_id=(d,), device_id_type=MESH)

    def own_line(src, src_row, dst, dst_row, recv):
        pltpu.make_async_copy(src.at[pl.ds(src_row, 1)], dst.at[pl.ds(dst_row, 1)], recv.at[0]).start()

    def plane_peers(body):
        @pl.loop(1, plane)
        def _(step):
            d = partner(1, step)
            for j in range(share_rows):
                body(step * share_rows + j, d, lax.rem(d, plane) * share_rows + j, low * share_rows + j, j)

    def scatter(q, d, theirs, ours, j):
        return line_copy(part_s, theirs, part_r, ours, s_part, v_part, q, d)

    def line_peers(body):
        for quarter in (0, 3, 2):
            d = partner(quarter, 0)
            for j in range(share_rows):
                body(quarter * share_rows + j, d, j)

    def exchange(q, d, j):
        return line_copy(mid_s, j, mid_r, high * share_rows + j, s_mid, v_mid, q, d)

    def gather(q, d, theirs, ours, j):
        return line_copy(sum_s, j, gg_ref, ours, s_sum, v_sum, q, d)

    plane_peers(lambda *a: scatter(*a).start())
    for j in range(share_rows):
        own_line(part_s, low * share_rows + j, part_r, low * share_rows + j, v_part)
    backward(late)
    settle(part_r, v_part.at[0], pl.ds(0, n))
    fold = part_r[0:8, :] + part_r[8:16, :] + part_r[16:24, :] + part_r[24:32, :]
    mid_s[0:4, :] = fold[0:4] + fold[4:8]
    line_peers(lambda *a: exchange(*a).start())
    for j in range(share_rows):
        own_line(mid_s, j, mid_r, high * share_rows + j, v_mid)
    each_partner(everyone, lambda q, d: one_row(dots_s, dots_r, q, s_dot, v_dot, q, d).start())
    own_row(dots_s, dots_r, plane, v_dot)
    send_back(late, ((3, 0, plane),))
    gw1[...] = dot(xet[...], gpre[...]).astype(BF16)
    gw2[...] = dot(act[...], gy[...], TN).astype(BF16)

    settle(mid_r, v_mid.at[0], pl.ds(0, 16))
    fold = mid_r[0:8, :] + mid_r[8:16, :]
    sum_s[0:4, :] = fold[0:4] + fold[4:8]
    plane_peers(lambda *a: gather(*a).start())
    for j in range(share_rows):
        own_line(sum_s, j, gg_ref, low * share_rows + j, v_sum)

    settle(dots_r, v_dot.at[0], pl.ds(0, n))
    all_dots = dots_r[...]
    d1 = jnp.sum(dot(all_dots, hot1, TN, precision=exact) * at1, axis=0, keepdims=True)
    d2 = jnp.sum(dot(all_dots, hot2, TN, precision=exact) * at2, axis=0, keepdims=True)
    apart = d1.astype(BF16).astype(F32) - d2.astype(BF16).astype(F32)
    glog = (aux_log + (mix * apart) * (hot1 - hot2)).astype(BF16)

    both = jnp.sum(jnp.where(lane_1 == 96, total, 0.0), axis=1, keepdims=True)
    both = both + jnp.sum(jnp.where(lane_1 == 16, jnp.sum(all_dots, axis=0, keepdims=True), 0.0), axis=1, keepdims=True)
    aux = jnp.sum(frac * mean_prob, axis=0, keepdims=True) * n
    loss_ref[...] = jnp.broadcast_to(both / numel + ALPHA * aux, loss_ref.shape)
    out = r_ref[...].astype(F32) + dot(glog, wg_ref[...], TN)
    each_partner(everyone, lambda q, d: one_row(rows_s, rows_r, d, s_row, v_row, q, d).wait_send())
    each_partner(everyone, lambda q, d: one_row(dots_s, dots_r, q, s_dot, v_dot, q, d).wait_send())
    plane_peers(lambda *a: scatter(*a).wait_send())
    line_peers(lambda *a: exchange(*a).wait_send())

    def sent(ref, sem, groups_sent):
        for c in groups_sent:
            start, size = span[c]
            settle(ref, sem.at[c], pl.ds(own + rows, size - rows) if c == near else pl.ds(start, size))

    sent(sx, s_x, (early, near, late))
    sent(sr, s_r, (early, near, late))
    sent(gs, s_g, (early, near))
    for c in (near, early):
        start, size = span[c]
        settle(gback, v_g.at[c], group_at(c))
        out = out + dot(comb[:, start:start + size], gback[group_at(c), :])
    plane_peers(lambda *a: gather(*a).wait_send())
    settle(gg_ref, v_sum.at[0], pl.ds(0, n))
    sent(gs, s_g, (late,))
    start, size = span[late]
    settle(gback, v_g.at[late], group_at(late))
    gx_ref[...] = (out + dot(comb[:, start:start + size], gback[group_at(late), :])).astype(BF16)


def solution(mesh):
    n = mesh.shape['ep']

    def layer_body(x_loc, r_loc, w_gate, w_in_loc, w_out_loc, first_ids, second_ids, keep_ids):
        groups, seq, hidden = x_loc.shape
        cap = 2 * seq // w_gate.shape[1]
        ff = w_in_loc.shape[2]
        tokens = groups * seq
        slots = n * groups * cap
        vmem = pl.BlockSpec(memory_space=pltpu.VMEM)
        hbm = pl.BlockSpec(memory_space=pltpu.HBM)
        dma = pltpu.SemaphoreType.DMA
        out = pl.pallas_call(
            functools.partial(layer_kernel, n, cap, seq),
            name='moe_layer',
            out_shape=(
                pltpu.VMEM((8, 128), F32),
                pltpu.VMEM((tokens, hidden), BF16),
                pltpu.VMEM((n, hidden), F32),
                pltpu.VMEM((hidden, ff), BF16),
                pltpu.VMEM((ff, hidden), BF16),
            ),
            in_specs=[hbm] * 8,
            out_specs=(vmem,) * 5,
            scratch_shapes=[
                pltpu.VMEM((groups, seq), jnp.int32),
                pltpu.VMEM((groups, seq), jnp.int32),
                pltpu.VMEM((groups, seq), jnp.int32),
                pltpu.VMEM((tokens, hidden), BF16),
                pltpu.VMEM((tokens, hidden), BF16),
                pltpu.VMEM((n, hidden), BF16),
                pltpu.VMEM((hidden, ff), BF16),
                pltpu.VMEM((ff, hidden), BF16),
                pltpu.VMEM((slots, hidden), BF16),
                pltpu.VMEM((slots, hidden), BF16),
                pltpu.VMEM((slots, hidden), BF16),
                pltpu.VMEM((slots, hidden), BF16),
                pltpu.VMEM((slots, hidden), BF16),
                pltpu.VMEM((slots, ff), BF16),
                pltpu.VMEM((slots, ff), BF16),
                pltpu.VMEM((slots, hidden), BF16),
                pltpu.VMEM((slots, hidden), BF16),
                pltpu.VMEM((n, 128), F32),
                pltpu.VMEM((n, 128), F32),
                pltpu.VMEM((n, 128), F32),
                pltpu.VMEM((n, 128), F32),
                pltpu.VMEM((n, hidden), F32),
                pltpu.VMEM((n, hidden), F32),
                pltpu.VMEM((8, hidden), F32),
                pltpu.VMEM((16, hidden), F32),
                pltpu.VMEM((8, hidden), F32),
                pltpu.VMEM((slots, ff), F32),
                pltpu.VMEM((slots, hidden), BF16),
                pltpu.VMEM((hidden, slots), BF16),
                dma((8,)),
                dma((3,)), dma((3,)), dma((3,)), dma((n,)), dma((n,)), dma((n,)), dma((16,)), dma((n,)),
                dma((3,)), dma((3,)), dma((3,)), dma((1,)), dma((1,)), dma((1,)), dma((1,)), dma((1,)),
            ],
            compiler_params=pltpu.CompilerParams(collective_id=0, has_side_effects=True, vmem_limit_bytes=44 * 1024 * 1024),
        )(*(pltpu.with_memory_space_constraint(a, pltpu.HBM) for a in (
            first_ids, second_ids, keep_ids, x_loc.reshape(tokens, hidden), r_loc.reshape(tokens, hidden), w_gate.T, w_in_loc[0], w_out_loc[0])))
        loss, gx, gg, gw1, gw2 = pl.pallas_call(
            write_kernel,
            name='write_results',
            out_shape=(
                jax.ShapeDtypeStruct((1, 1), F32),
                jax.ShapeDtypeStruct((tokens, hidden), BF16),
                jax.ShapeDtypeStruct((n, hidden), F32),
                jax.ShapeDtypeStruct((hidden, ff), BF16),
                jax.ShapeDtypeStruct((ff, hidden), BF16),
            ),
            in_specs=[vmem] * 5,
            out_specs=(pl.BlockSpec(memory_space=pltpu.SMEM), hbm, hbm, hbm, hbm),
            scratch_shapes=[dma((4,))],
            compiler_params=pltpu.CompilerParams(vmem_limit_bytes=2 * 1024 * 1024),
        )(*(pltpu.with_memory_space_constraint(a, pltpu.VMEM) for a in out))
        return loss.reshape(()), gx.reshape(x_loc.shape), gw1[None], gw2[None], gg.T

    row_spec = P('ep', None, None)
    id_spec = P('ep', None)
    return jax.shard_map(layer_body, mesh=mesh, in_specs=(row_spec, row_spec, P(None, None), row_spec, row_spec, id_spec, id_spec, id_spec), out_specs=(P(), row_spec, row_spec, row_spec, P(None, None)), check_vma=False)
```
